256 devices in a mesh: groups: 2 (over z), section: 2 (over core), expert: 64 (over y, x).
Axes of the slice: x: 8, y: 8, z: 2, core: 2. Of those that a mesh axis runs over, the one named last changes fastest.
The devices are a block of a 8x8x16 slice.
Arguments:
- tokens: bfloat16 [2, 1024, 6144], P(None, ('groups', 'expert')), parts along dimension 1, may hold values from -6 to 6
- expert_ids: int32 [2, 2, 1024, 2], P('section', None, ('groups', 'expert')), parts along dimension 2, may hold values from 0 to 7, all different within a row; in each aligned block of 8 rows (0 to 7, 8 to 15, ..., all dimensions but the last counted through in order) at most 4 rows name the same one
- norm_gain: bfloat16 [2, 6144], P('section'), may hold values from 0.25 to 1.75
- router: bfloat16 [2, 6144, 8], P('section'), may hold values from -0.078125 to 0.078125
- w_gate: bfloat16 [2, 6144, 16384], P('section', None, 'expert'), may hold values from -0.078125 to 0.078125
- w_up: bfloat16 [2, 6144, 16384], P('section', None, 'expert'), may hold values from -0.078125 to 0.078125
- w_down: bfloat16 [2, 16384, 6144], P('section', 'expert'), may hold values from -0.0625 to 0.0625
Outputs:
- mixed: bfloat16 [2, 1024, 6144], P('section', ('groups', 'expert')), parts along dimension 1
The draws below stay inside these ranges and needn't reach their ends.
There are 2 independent parts, one for each index of `groups`. The reference program is written for one: setup_inputs(seed, part) draws one part's arguments, and reference() takes and returns one part's arrays. A program takes and returns all parts, laid end to end along the dimension named above; an argument that names none is the same for every part. Nothing has to cross between parts.
Inputs may be any that keep to these rules, and one draw needn't show every extreme that they name: `expert_ids`: in each aligned block of 8 rows (one index of expert, one micro-batch, one layer) no expert is named by more than 4 of the pairs; a token's two ids differ.
All inputs are finite; a program needn't handle non-finite values.
Results may differ from the reference program's by a relative error of at most 0.0055.
Values may be sent and summed in bfloat16 or wider, within the bound.
A program may use at most 128 MiB of HBM per device.

```python
import math
import jax
import jax.numpy as jnp
import numpy as np
from jax import lax

D = 6144
FF_WIN = 8192
NEXP = 8
TOPK = 2
E_WIN = 2
TOK_DEV = 8
CAP = 4
SPLIT = 32
FF_DEV = 256
MICRO = 2
LAYERS = 2
TOKENS = 512
N_EXPERT = 64


def block_scale(own_key, extent, cuts, low, largest):
    def one(axis_at, parts):
        steps = jax.random.uniform(jax.random.fold_in(jax.random.fold_in(own_key, 6), axis_at), (parts,), jnp.float32, low / len(cuts), largest / len(cuts))
        return jnp.repeat(jnp.exp(steps), extent[axis_at] // parts).reshape((-1,) + (1,) * (len(extent) - axis_at - 1))

    level = one(*cuts[0])
    for cut in cuts[1:]:
        level = level * one(*cut)
    return level


def shared_out(rng, own, number, rows, amount, top, bound, skew):
    ranking = jax.random.permutation(rng, amount)
    crowded, common = shares(amount, rows * top, bound, skew, True), shares(amount, rows * top, bound, skew, False)
    places = jnp.arange(amount)

    def named(lengths, turn):
        used = int((lengths > 0).sum())
        fixed = max(1, used // 4)
        passed = fixed + (places - fixed + turn * (used - fixed)) % max(1, amount - fixed)
        return jnp.zeros((amount,), jnp.int32).at[ranking[jnp.where(places < fixed, places, passed)]].set(jnp.asarray(lengths, jnp.int32))

    lengths = jnp.where(number % 4 == 0, named(crowded, number // 4), named(common, number - number // 4 - 1))
    mixed = jax.random.permutation(jax.random.fold_in(own, 3), amount)
    source_of, sink = mixed[0:amount // 2 * 2:2], mixed[1:amount // 2 * 2:2]
    margin = jnp.minimum(lengths[source_of] - 1, bound - lengths[sink]) // 2
    margin = jnp.where((source_of == ranking[0]) | (sink == ranking[0]) | (lengths[sink] == 0), 0, jnp.maximum(margin, 0))
    passed = jax.random.randint(jax.random.fold_in(own, 4), (amount // 2,), 0, 1 << 20) % (margin + 1)
    lengths = lengths.at[source_of].add(-passed).at[sink].add(passed)
    labels = jnp.searchsorted(jnp.cumsum(lengths), jnp.arange(rows * top), side="right").astype(jnp.int32)
    listing = labels.reshape(top, rows).T
    listing = listing[jax.random.permutation(jax.random.fold_in(own, 1), rows)]
    turn = jax.random.randint(jax.random.fold_in(own, 2), (rows, 1), 0, top)
    return jnp.take_along_axis(listing, (jnp.arange(top)[None, :] + turn) % top, axis=1)


def shares(amount, total, reach, skew, full):
    loads = [(1 << 20) // math.isqrt(rank ** skew) + 1 for rank in range(1, amount + 1)]
    largest = reach if full else min(reach, max(-(-total // amount), total * loads[0] // sum(loads)))
    least = 1 if total - largest >= amount - 1 else 0
    counts, rest = [largest] + [least] * (amount - 1), total - largest - least * (amount - 1)
    while rest > 0:
        candidates = [i for i in range(1, amount) if counts[i] < largest] or [i for i in range(1, amount) if counts[i] < reach]
        pool, left = sum([loads[i] for i in candidates]), rest
        for i in candidates:
            extra = min(reach - counts[i], max(1, left * loads[i] // pool), rest)
            counts[i] = counts[i] + extra
            rest = rest - extra
    return np.array(counts)


def normal_values(stream_key, shape, spread, reach, shards=(), kind=jnp.bfloat16):
    level = block_scale(stream_key, shape, shards, -0.22, 0.18) if shards else 1.0
    result = jax.random.normal(stream_key, shape, jnp.float32) * spread * level
    return jnp.minimum(jnp.maximum(result, -reach), reach).astype(kind)


def setup_inputs(seed: int = 0, part: int = 0) -> dict:
    keys = jax.random.split(jax.random.key(seed), 8)
    part_keys = jax.random.split(jax.random.fold_in(keys[7], part), 8)
    tokens = normal_values(part_keys[0], (MICRO, TOKENS, D), 1.0, 6.0, ((1, 64),))
    expert_ids_keys = jax.random.split(jax.random.fold_in(part_keys[1], 1), LAYERS * MICRO * TOKENS // TOK_DEV)
    expert_ids_turns = jax.random.permutation(jax.random.fold_in(part_keys[1], 3), LAYERS * MICRO * TOKENS // TOK_DEV)
    expert_ids = jax.vmap(lambda own, number: shared_out(jax.random.fold_in(part_keys[1], 2), own, number, TOK_DEV, NEXP, TOPK, CAP, 2))(expert_ids_keys, expert_ids_turns).reshape((LAYERS, MICRO, TOKENS, TOPK))
    norm_gain = jnp.clip(1.0 + 0.15 * jax.random.normal(keys[2], (LAYERS, D), jnp.float32), 0.25, 1.75).astype(jnp.bfloat16)
    router = normal_values(keys[3], (LAYERS, D, NEXP), D ** -0.5, 0.078125, ((0, 2),))
    w_gate = normal_values(keys[4], (LAYERS, D, E_WIN * FF_WIN), D ** -0.5, 0.078125, ((0, 2), (2, 64)))
    w_up = normal_values(keys[5], (LAYERS, D, E_WIN * FF_WIN), D ** -0.5, 0.078125, ((0, 2), (2, 64)))
    w_down = normal_values(keys[6], (LAYERS, E_WIN * FF_WIN, D), FF_WIN ** -0.5, 0.0625, ((0, 2), (1, 64)))
    return {"tokens": tokens, "expert_ids": expert_ids, "norm_gain": norm_gain, "router": router, "w_gate": w_gate, "w_up": w_up, "w_down": w_down}


epsilon = 1e-05

def normalize(stream, gain):
    values = stream.astype(jnp.float32)
    scale = lax.rsqrt(lax.optimization_barrier(jnp.mean(values * values, axis=-1, keepdims=True)) + epsilon)
    return (values * scale * gain.astype(jnp.float32)).astype(jnp.bfloat16)

def route(normed, chosen_ids, router_matrix):
    logits = jnp.dot(normed, router_matrix, preferred_element_type=jnp.float32)
    chosen_hot = (chosen_ids[..., None] == jnp.arange(NEXP, dtype=jnp.int32)).astype(jnp.float32)
    chosen = lax.optimization_barrier(jnp.sum(chosen_hot * logits[:, None, :], axis=-1))
    first = jax.nn.sigmoid(chosen[:, 0] - chosen[:, 1])
    second = jax.nn.sigmoid(chosen[:, 1] - chosen[:, 0])
    gates = jnp.stack([first, second], axis=1)
    flat = chosen_hot.reshape(-1, NEXP)
    before = jnp.cumsum(flat, axis=0) - flat
    position = lax.optimization_barrier(jnp.sum(before * flat, axis=-1))
    slot_hot = (position[:, None] == jnp.arange(CAP, dtype=jnp.float32)).astype(jnp.float32)
    assign = (flat[:, :E_WIN, None] * slot_hot[:, None, :]).reshape(-1, TOPK, E_WIN * CAP)
    pick = lax.optimization_barrier(jnp.sum(assign, axis=1))
    weights = lax.optimization_barrier(jnp.sum(gates[:, :, None] * assign, axis=1))
    return (pick, weights)

def layer(stream, chosen_ids, gain, router_matrix, gate_matrix, up_matrix, down_matrix):
    normed = normalize(stream, gain)
    blocks = normed.reshape(N_EXPERT, TOK_DEV, D)
    id_blocks = chosen_ids.reshape(N_EXPERT, TOK_DEV, TOPK)
    pick, weights = jax.vmap(lambda rows_in, ids_in: route(rows_in, ids_in, router_matrix))(blocks, id_blocks)
    packed = jnp.einsum('ntc,ntd->ncd', pick, blocks.astype(jnp.float32)).astype(jnp.bfloat16)

    def one_slice(total, device_index):
        expert_index = device_index // SPLIT
        rows = lax.dynamic_slice_in_dim(packed, (expert_index * CAP).astype(jnp.int32), CAP, 1).reshape(N_EXPERT * CAP, D)
        start = (device_index * FF_DEV).astype(jnp.int32)
        gate_part = lax.dynamic_slice_in_dim(gate_matrix, start, FF_DEV, 1)
        up_part = lax.dynamic_slice_in_dim(up_matrix, start, FF_DEV, 1)
        down_part = lax.dynamic_slice_in_dim(down_matrix, start, FF_DEV, 0)
        gate_value = jnp.dot(rows, gate_part, preferred_element_type=jnp.float32)
        up_value = jnp.dot(rows, up_part, preferred_element_type=jnp.float32)
        hidden = (jax.nn.silu(gate_value) * up_value).astype(jnp.bfloat16)
        term = jnp.dot(hidden, down_part, preferred_element_type=jnp.float32).astype(jnp.bfloat16)
        term = term.astype(jnp.float32).reshape(N_EXPERT, CAP, D)
        select = (jnp.arange(E_WIN, dtype=jnp.int32) == expert_index).astype(jnp.float32)
        return (total + select[None, :, None, None] * term[:, None, :, :], None)
    start_total = jnp.zeros((N_EXPERT, E_WIN, CAP, D), jnp.float32)
    total, unused = lax.scan(one_slice, start_total, jnp.arange(N_EXPERT, dtype=jnp.int32))
    expert_out = total.reshape(N_EXPERT, E_WIN * CAP, D)
    moe = jnp.einsum('ntc,ncd->ntd', weights, expert_out, precision=lax.Precision.HIGHEST)
    return (stream.astype(jnp.float32) + moe.reshape(TOKENS, D)).astype(jnp.bfloat16)

def reference(tokens, expert_ids, norm_gain, router, w_gate, w_up, w_down):
    results = []
    for micro_index in range(MICRO):
        stream = tokens[micro_index]
        for layer_index in range(LAYERS):
            stream = layer(stream, expert_ids[layer_index, micro_index], norm_gain[layer_index], router[layer_index], w_gate[layer_index], w_up[layer_index], w_down[layer_index])
        results.append(stream)
    return jnp.stack(results)
```

```python
import functools
import math

import jax
import jax.numpy as jnp
from jax import lax
from jax.experimental import pallas as pl
from jax.experimental.pallas import tpu as pltpu
from jax.sharding import PartitionSpec as P

E_WIN = 2
CAP = 4
PIECES = 4
EPS = 1e-05
MESH = pl.DeviceIdType.MESH
F32, BF16 = jnp.float32, jnp.bfloat16


def bits(value, low, count):
    return lax.bitwise_and(lax.shift_right_logical(value, low), (1 << count) - 1)


def iota(shape, dim):
    return lax.broadcasted_iota(jnp.int32, shape, dim)


def one_hot(condition):
    return jnp.where(condition, 1.0, 0.0).astype(BF16)


def swap(rows, high, low, tail):
    to, frm = iota((rows, rows), 0), iota((rows, rows), 1)
    to_l, to_h = bits(to, tail + high, low), bits(to, tail, high)
    frm_h, frm_l = bits(frm, tail + low, high), bits(frm, tail, low)
    same = (bits(to, 0, tail) == bits(frm, 0, tail)) & (to_l == frm_l) & (to_h == frm_h)
    return one_hot(same)


def dot(a, b, **kw):
    return jnp.dot(a, b, preferred_element_type=F32, **kw)


def dot_t(a, b):
    return lax.dot_general(a, b, (((1,), (1,)), ((), ())), preferred_element_type=F32)


def kernel(side, tokens, ids, gain, router, w_gate, w_up, w_down, out,
           stream, normed, ids_all, gain_all, router_all, gate_all, up_all, down_all,
           pack_a, pack_b, unit_a, unit_b, ga, gb, ta, tb, sb, ra, rb, wa, wb, va, vb,
           own_sem, param_sem, param_send, dir_send, dir_recv, ring_send, ring_recv,
           back_send, back_recv, sum_send, sum_recv):
    lg = side.bit_length() - 1
    width = stream.shape[1]
    ca, cb = ga.shape[-1], gb.shape[-1]
    base_b = PIECES * ca
    s = lax.axis_index("section")
    me = lax.axis_index("expert")
    y, x = me // side, me % side
    expert = y // (side // E_WIN)
    bundle = side * CAP

    def at(yy, xx):
        return {"expert": yy * side + xx}

    other = {"section": 1 - s}
    params = ((gain, gain_all), (router, router_all), (w_gate, gate_all), (w_up, up_all), (w_down, down_all))

    def remote(src, dst, send, recv, device):
        return pltpu.make_async_remote_copy(src_ref=src, dst_ref=dst, send_sem=send, recv_sem=recv,
                                            device_id=device, device_id_type=MESH)

    token_copy = pltpu.make_async_copy(tokens.at[s], stream, own_sem)
    token_copy.start()
    pltpu.make_async_copy(ids.at[s], ids_all.at[s], param_sem.at[5, s]).start()
    for kind, (src, dst) in enumerate(params):
        pltpu.make_async_copy(src.at[0], dst.at[s], param_sem.at[kind, s]).start()

    barrier = pltpu.get_barrier_semaphore()
    pl.semaphore_signal(barrier, inc=1, device_id=other, device_id_type=MESH)
    for step in range(1, side):
        pl.semaphore_signal(barrier, inc=1, device_id=at(y, (x + step) % side), device_id_type=MESH)
        pl.semaphore_signal(barrier, inc=1, device_id=at((y + step) % side, x), device_id_type=MESH)
    pl.semaphore_wait(barrier, 2 * side - 1)

    sends = [remote(ids.at[1 - s], ids_all.at[s], param_send.at[5], param_sem.at[5, s], other)]
    for kind, (src, dst) in enumerate(params):
        sends.append(remote(src.at[0], dst.at[s], param_send.at[kind], param_sem.at[kind, s], other))
    for copy in sends:
        copy.start()

    def param_wait(kind, layer):
        src, dst = params[kind]
        pltpu.make_async_copy(src.at[0], dst.at[layer], param_sem.at[kind, layer]).wait()

    sb[...] = jnp.zeros_like(sb)
    token_copy.wait()

    def forward(piece):
        return 1 if piece < PIECES // 2 else -1

    def place(k):
        return x if k < PIECES else y

    def beside(k):
        go = forward(k % PIECES)
        return at(y, (x + go) % side) if k < PIECES else at((y + go) % side, x)

    def from_place(k, steps):
        return (place(k) + 8 * side - forward(k % PIECES) * steps) % side

    def gathered(k, layer, slot):
        return ga.at[layer, slot, k] if k < PIECES else gb.at[layer, slot, k - PIECES]

    def running(k, layer, step):
        return ra.at[layer, step, k] if k < PIECES else rb.at[layer, step, k - PIECES]

    streams = range(2 * PIECES)

    def one_layer(layer, carry):
        pltpu.make_async_copy(ids.at[s], ids_all.at[layer], param_sem.at[5, layer]).wait()
        param_wait(0, layer)
        param_wait(1, layer)
        values = stream[...].astype(F32)
        scale = lax.rsqrt(jnp.mean(values * values, axis=-1, keepdims=True) + EPS)
        normed[...] = (values * scale * gain_all[layer].astype(F32)).astype(BF16)
        id_block = ids_all[layer]
        rows8 = id_block.shape[0]
        lanes = iota((rows8, 128), 1)
        named = [id_block[:, k:k + 1] for k in range(2)]
        hot = [jnp.where(lanes == n, 1.0, 0.0) for n in named]
        earlier = jnp.where(iota((rows8, rows8), 0) > iota((rows8, rows8), 1), 1.0, 0.0)
        before = dot(earlier.astype(BF16), (hot[0] + hot[1]).astype(BF16))
        code = [jnp.sum(h * before, axis=-1, keepdims=True) + n.astype(F32) * CAP
                for h, n in zip(hot, named)]
        lane_f = lanes.astype(F32)
        joint = sum(jnp.where(lane_f == c, 1.0, 0.0) for c in code).astype(BF16)
        r = iota((32, 128), 0)
        c = iota((32, 128), 1)
        code_a = bits(r, 4, 1) * CAP + bits(r, 0, 2)
        code_b = bits(r, 0, 3)
        pick_a = dot_t(one_hot(c == code_a), joint)
        pick_b = dot_t(one_hot(c == code_b), joint)
        rr = iota((32, rows8), 0)
        packed_a = jnp.zeros((32, ca), F32)
        packed_b = jnp.zeros((32, cb), F32)
        for q in range(PIECES):
            mine_a = jnp.where(bits(rr, 2, 2) == q, pick_a, 0.0).astype(BF16)
            packed_a += dot(mine_a, normed[:, q * ca:(q + 1) * ca])
            mine_b = jnp.where(bits(rr, 3, 2) == q, pick_b, 0.0).astype(BF16)
            packed_b += dot(mine_b, normed[:, base_b + q * cb:base_b + (q + 1) * cb])
        pack_a[...] = packed_a.astype(BF16).reshape(E_WIN, PIECES * CAP, ca)
        pack_b[...] = packed_b.astype(BF16)
        unit_a[layer, y] = pack_a[expert]
        unit_b[layer, x] = pack_b[...]

        def direct_a(step):
            to = (y + step) % side
            return remote(pack_a.at[to // (side // E_WIN)], unit_a.at[layer, y], dir_send.at[0, step],
                          dir_recv.at[layer, 0, step], at(to, x))

        def direct_b(step):
            return remote(pack_b, unit_b.at[layer, x], dir_send.at[1, step],
                          dir_recv.at[layer, 1, step], at(y, (x + step) % side))

        for step in range(1, side):
            direct_a(step).start()
            direct_b(step).start()

        logits = dot_t(normed[...], router_all[layer])
        chosen = [jnp.sum(h[:, :logits.shape[1]] * logits, axis=-1, keepdims=True) for h in hot]
        gates = [jax.nn.sigmoid(chosen[0] - chosen[1]), jax.nn.sigmoid(chosen[1] - chosen[0])]

        for step in range(1, side):
            direct_a(step).wait()
        ga[layer, x] = dot(swap(side * 16, lg, 2, 2), unit_a[layer].reshape(side * 16, ca)).astype(BF16).reshape(
            PIECES, bundle, ca)

        def hop(k, step):
            slot = from_place(k, step)
            ref = gathered(k, layer, slot)
            return remote(ref, ref, ring_send.at[k], ring_recv.at[layer, k, step], beside(k))

        for k in range(PIECES):
            hop(k, 0).start()
        for step in range(1, side):
            direct_b(step).wait()
        gb[layer, y] = dot(swap(side * 32, lg, 3, 2), unit_b[layer].reshape(side * 32, cb)).astype(BF16).reshape(
            PIECES, 2 * bundle, cb)
        for k in range(PIECES, 2 * PIECES):
            hop(k, 0).start()

        def ring_step(step, c):
            for k in streams:
                hop(k, step - 1).wait()
                hop(k, step).start()
            return c

        lax.fori_loop(1, side - 1, ring_step, 0)
        for k in streams:
            hop(k, side - 2).wait()

        for kind in (2, 3, 4):
            param_wait(kind, layer)
        rows = side * bundle
        ff = gate_all.shape[-1]
        order = swap(rows, lg, lg, 2)

        def part_a(q, carry):
            g, u = carry
            lhs = ga[layer, :, q].reshape(rows, ca)
            at_rows = pl.ds(pl.multiple_of(q * ca, ca), ca)
            return g + dot(lhs, gate_all[layer, at_rows]), u + dot(lhs, up_all[layer, at_rows])

        def part_b(q, carry):
            g, u = carry
            lhs = gb[layer, :, q, pl.ds(pl.multiple_of(expert * bundle, bundle), bundle)].reshape(rows, cb)
            lhs = dot(order, lhs).astype(BF16)
            at_rows = pl.ds(pl.multiple_of(base_b + q * cb, cb), cb)
            return g + dot(lhs, gate_all[layer, at_rows]), u + dot(lhs, up_all[layer, at_rows])

        zero = jnp.zeros((rows, ff), F32)
        sums = lax.fori_loop(0, PIECES, part_a, (zero, zero))
        g, u = lax.fori_loop(0, PIECES, part_b, sums)
        hidden = (g * jax.nn.sigmoid(g) * u).astype(BF16)
        hidden_b = dot(order, hidden).astype(BF16)
        for q in range(PIECES):
            term = dot(hidden, down_all[layer, :, q * ca:(q + 1) * ca]).astype(BF16)
            ta[q] = term.reshape(side, bundle, ca)
            term = dot(hidden_b, down_all[layer, :, base_b + q * cb:base_b + (q + 1) * cb]).astype(BF16)
            tb[q] = term.reshape(side, bundle, cb)
        own_half = pl.ds(pl.multiple_of(expert * bundle, bundle), bundle)

        def pass_on(k, step):
            if step is None:
                src, step = (ta.at[k, from_place(k, 1)] if k < PIECES else sb.at[k - PIECES]), 0
            else:
                src = running(k, layer, step)
            return remote(src, running(k, layer, step + 1), sum_send.at[k], sum_recv.at[layer, k, step + 1],
                          beside(k))

        def add_own(k, step):
            slot = from_place(k, step + 1)
            if k < PIECES:
                ra[layer, step, k] = (ra[layer, step, k].astype(F32) + ta[k, slot].astype(F32)).astype(BF16)
            else:
                q = k - PIECES
                rb[layer, step, q, own_half] = (
                    rb[layer, step, q, own_half].astype(F32) + tb[q, slot].astype(F32)).astype(BF16)

        for k in streams:
            if k >= PIECES:
                sb[k - PIECES, own_half] = tb[k - PIECES, from_place(k, 1)]
            pass_on(k, None).start()
        for k in streams:
            pass_on(k, None).wait()
            add_own(k, 1)
            pass_on(k, 1).start()

        def sum_step(step, c):
            for k in streams:
                pass_on(k, step - 1).wait()
                add_own(k, step)
                pass_on(k, step).start()
            return c

        lax.fori_loop(2, side - 1, sum_step, 0)
        for k in streams:
            pass_on(k, side - 2).wait()
            add_own(k, side - 1)

        last = side - 1
        wa[...] = dot(swap(side * 16, 2, lg, 2), ra[layer, last].reshape(side * 16, ca)).astype(BF16).reshape(
            side, PIECES * CAP, ca)
        wb[...] = dot(swap(side * 32, 3, lg, 2), rb[layer, last].reshape(side * 32, cb)).astype(BF16).reshape(
            side, PIECES * 2 * CAP, cb)
        va[layer, y] = wa[y]
        vb[layer, x] = wb[x]

        def back_a(step):
            to = (y + step) % side
            return remote(wa.at[to], va.at[layer, y], back_send.at[0, step], back_recv.at[layer, 0, step], at(to, x))

        def back_b(step):
            to = (x + step) % side
            return remote(wb.at[to], vb.at[layer, x], back_send.at[1, step], back_recv.at[layer, 1, step], at(y, to))

        for step in range(1, side):
            back_a(step).start()
            back_b(step).start()
        for step in range(1, side):
            back_a(step).wait()
            back_b(step).wait()

        half = side // E_WIN
        out_a = jnp.concatenate(
            [sum(va[layer, n * half + j].astype(F32) for j in range(half)) for n in range(E_WIN)], axis=0)
        out_b = sum(vb[layer, j].astype(F32) for j in range(side))
        lane = iota((rows8, 32), 1)
        code_a = (bits(lane, 4, 1) * CAP + bits(lane, 0, 2)).astype(F32)
        code_b = bits(lane, 0, 3).astype(F32)
        weight_a = sum(jnp.where(code_a == c, g_, 0.0) for c, g_ in zip(code, gates))
        weight_b = sum(jnp.where(code_b == c, g_, 0.0) for c, g_ in zip(code, gates))
        for q in range(PIECES):
            for weight, which, value, begin, wide in (
                    (weight_a, bits(lane, 2, 2), out_a, q * ca, ca),
                    (weight_b, bits(lane, 3, 2), out_b, base_b + q * cb, cb)):
                moe = dot(jnp.where(which == q, weight, 0.0), value, precision=lax.Precision.HIGHEST)
                columns = slice(begin, begin + wide)
                stream[:, columns] = (stream[:, columns].astype(F32) + moe).astype(BF16)
        return carry

    lax.fori_loop(0, 2, one_layer, 0)
    out[0] = stream[...]
    for copy in sends:
        copy.wait_send()


def body(tokens, expert_ids, norm_gain, router, w_gate, w_up, w_down):
    side = math.isqrt(lax.axis_size("expert"))
    block, width = tokens.shape[1:]
    ff = w_gate.shape[-1]
    ca = width * 2 // 3 // PIECES
    cb = width // 3 // PIECES
    bundle = side * CAP
    ids = jnp.pad(expert_ids[0], ((0, 0), (0, 0), (0, 128 - expert_ids.shape[-1])))
    router_t = jnp.swapaxes(router, 1, 2)
    gain = norm_gain[:, None, :]
    dma = pltpu.SemaphoreType.DMA
    hbm = pl.BlockSpec(memory_space=pl.ANY)
    scratch = [
        pltpu.VMEM((block, width), BF16),
        pltpu.VMEM((block, width), BF16),
        pltpu.VMEM((2, block, 128), jnp.int32),
        pltpu.VMEM((2, 1, width), BF16),
        pltpu.VMEM((2, router.shape[-1], width), BF16),
        pltpu.VMEM((2, width, ff), BF16),
        pltpu.VMEM((2, width, ff), BF16),
        pltpu.VMEM((2, ff, width), BF16),
        pltpu.VMEM((E_WIN, PIECES * CAP, ca), BF16),
        pltpu.VMEM((PIECES * E_WIN * CAP, cb), BF16),
        pltpu.VMEM((2, side, PIECES * CAP, ca), BF16),
        pltpu.VMEM((2, side, PIECES * E_WIN * CAP, cb), BF16),
        pltpu.VMEM((2, side, PIECES, bundle, ca), BF16),
        pltpu.VMEM((2, side, PIECES, E_WIN * bundle, cb), BF16),
        pltpu.VMEM((PIECES, side, bundle, ca), BF16),
        pltpu.VMEM((PIECES, side, bundle, cb), BF16),
        pltpu.VMEM((PIECES, E_WIN * bundle, cb), BF16),
        pltpu.VMEM((2, side, PIECES, bundle, ca), BF16),
        pltpu.VMEM((2, side, PIECES, E_WIN * bundle, cb), BF16),
        pltpu.VMEM((side, PIECES * CAP, ca), BF16),
        pltpu.VMEM((side, PIECES * E_WIN * CAP, cb), BF16),
        pltpu.VMEM((2, side, PIECES * CAP, ca), BF16),
        pltpu.VMEM((2, side, PIECES * E_WIN * CAP, cb), BF16),
        dma,
        dma((6, 2)),
        dma((6,)),
        dma((2, side)),
        dma((2, 2, side)),
        dma((2 * PIECES,)),
        dma((2, 2 * PIECES, side)),
        dma((2, side)),
        dma((2, 2, side)),
        dma((2 * PIECES,)),
        dma((2, 2 * PIECES, side)),
    ]
    return pl.pallas_call(
        functools.partial(kernel, side),
        out_shape=jax.ShapeDtypeStruct((1, block, width), BF16),
        in_specs=[hbm] * 7,
        out_specs=pl.BlockSpec(memory_space=pltpu.VMEM),
        scratch_shapes=scratch,
        compiler_params=pltpu.CompilerParams(
            collective_id=0, has_side_effects=True, vmem_limit_bytes=60 * 1024 * 1024),
        name="moe_step",
    )(tokens, ids, gain, router_t, w_gate, w_up, w_down)


def solution(mesh):
    in_specs = (
        P(None, ("groups", "expert"), None),
        P("section", None, ("groups", "expert"), None),
        P("section", None),
        P("section", None, None),
        P("section", None, "expert"),
        P("section", None, "expert"),
        P("section", "expert", None),
    )
    out_specs = P("section", ("groups", "expert"), None)
    return jax.shard_map(body, mesh=mesh, in_specs=in_specs, out_specs=out_specs, check_vma=False)
```

```python
import functools
import math

import jax
import jax.numpy as jnp
from jax import lax
from jax.experimental import pallas as pl
from jax.experimental.pallas import tpu as pltpu
from jax.sharding import PartitionSpec as P

E_WIN = 2
CAP = 4
PIECES = 4
EPS = 1e-05
MESH = pl.DeviceIdType.MESH
F32, BF16 = jnp.float32, jnp.bfloat16


def bits(value, low, count):
    return lax.bitwise_and(lax.shift_right_logical(value, low), (1 << count) - 1)


def iota(shape, dim):
    return lax.broadcasted_iota(jnp.int32, shape, dim)


def one_hot(condition):
    return jnp.where(condition, 1.0, 0.0).astype(BF16)


def swap(rows, high, low, tail):
    to, frm = iota((rows, rows), 0), iota((rows, rows), 1)
    to_l, to_h = bits(to, tail + high, low), bits(to, tail, high)
    frm_h, frm_l = bits(frm, tail + low, high), bits(frm, tail, low)
    same = (bits(to, 0, tail) == bits(frm, 0, tail)) & (to_l == frm_l) & (to_h == frm_h)
    return one_hot(same)


def dot(a, b, **kw):
    return jnp.dot(a, b, preferred_element_type=F32, **kw)


def dot_t(a, b):
    return lax.dot_general(a, b, (((1,), (1,)), ((), ())), preferred_element_type=F32)


def kernel(side, tokens, ids, gain, router, w_gate, w_up, w_down, out,
           stream, normed, ids_all, gain_all, router_all, gate_all, up_all, down_all,
           pack_a, pack_b, unit_a, unit_b, ga, gb, ta, tb, sb, ra, rb, fa, fb, wa, wb, va, vb,
           own_sem, param_sem, param_send, dir_send, dir_recv, ring_send, ring_recv,
           back_send, back_recv, sum_send, sum_recv):
    lg = side.bit_length() - 1
    width = stream.shape[1]
    ca, cb = ga.shape[-1], gb.shape[-1]
    base_b = PIECES * ca
    s = lax.axis_index("section")
    me = lax.axis_index("expert")
    y, x = me // side, me % side
    expert = y // (side // E_WIN)
    bundle = side * CAP

    def at(yy, xx):
        return {"expert": yy * side + xx}

    other = {"section": 1 - s}
    params = ((gain, gain_all), (router, router_all), (w_gate, gate_all), (w_up, up_all), (w_down, down_all))

    def remote(src, dst, send, recv, device):
        return pltpu.make_async_remote_copy(src_ref=src, dst_ref=dst, send_sem=send, recv_sem=recv,
                                            device_id=device, device_id_type=MESH)

    token_copy = pltpu.make_async_copy(tokens.at[s], stream, own_sem)
    token_copy.start()
    pltpu.make_async_copy(ids.at[s], ids_all.at[s], param_sem.at[5, s]).start()
    for kind, (src, dst) in enumerate(params):
        pltpu.make_async_copy(src.at[0], dst.at[s], param_sem.at[kind, s]).start()

    barrier = pltpu.get_barrier_semaphore()
    pl.semaphore_signal(barrier, inc=1, device_id=other, device_id_type=MESH)
    for step in range(1, side):
        pl.semaphore_signal(barrier, inc=1, device_id=at(y, (x + step) % side), device_id_type=MESH)
        pl.semaphore_signal(barrier, inc=1, device_id=at((y + step) % side, x), device_id_type=MESH)
    pl.semaphore_wait(barrier, 2 * side - 1)

    sends = [remote(ids.at[1 - s], ids_all.at[s], param_send.at[5], param_sem.at[5, s], other)]
    for kind, (src, dst) in enumerate(params):
        sends.append(remote(src.at[0], dst.at[s], param_send.at[kind], param_sem.at[kind, s], other))
    for copy in sends:
        copy.start()

    def param_wait(kind, layer):
        src, dst = params[kind]
        pltpu.make_async_copy(src.at[0], dst.at[layer], param_sem.at[kind, layer]).wait()

    sb[...] = jnp.zeros_like(sb)
    token_copy.wait()

    half_way = side // 2

    def hops(k, go):
        return half_way if (k % PIECES < PIECES // 2) == (go > 0) else half_way - 1

    def place(k):
        return x if k < PIECES else y

    def beside(k, go):
        return at(y, (x + side + go) % side) if k < PIECES else at((y + side + go) % side, x)

    def shift(k, steps):
        return (place(k) + side + steps) % side

    order_of = [0, 2, 1, 3]
    streams = [(q + base, go) for q in order_of for base in (0, PIECES) for go in (1, -1)]

    def way(go):
        return 0 if go > 0 else 1

    def one_layer(layer, carry):
        pltpu.make_async_copy(ids.at[s], ids_all.at[layer], param_sem.at[5, layer]).wait()
        param_wait(0, layer)
        param_wait(1, layer)
        values = stream[...].astype(F32)
        scale = lax.rsqrt(jnp.mean(values * values, axis=-1, keepdims=True) + EPS)
        normed[...] = (values * scale * gain_all[layer].astype(F32)).astype(BF16)
        id_block = ids_all[layer]
        rows8 = id_block.shape[1]
        eye = one_hot(iota((rows8, rows8), 0) == iota((rows8, rows8), 1))
        id_block = dot_t(eye, id_block.astype(F32).astype(BF16))
        lanes = iota((rows8, 128), 1)
        named = [id_block[:, k:k + 1] for k in range(2)]
        lane_f = lanes.astype(F32)
        hot = [jnp.where(lane_f == n, 1.0, 0.0) for n in named]
        earlier = jnp.where(iota((rows8, rows8), 0) > iota((rows8, rows8), 1), 1.0, 0.0)
        before = dot(earlier.astype(BF16), (hot[0] + hot[1]).astype(BF16))
        code = [jnp.sum(h * before, axis=-1, keepdims=True) + n * CAP
                for h, n in zip(hot, named)]
        joint = sum(jnp.where(lane_f == c, 1.0, 0.0) for c in code).astype(BF16)
        r = iota((32, 128), 0)
        c = iota((32, 128), 1)
        code_a = bits(r, 4, 1) * CAP + bits(r, 0, 2)
        code_b = bits(r, 0, 3)
        pick_a = dot_t(one_hot(c == code_a), joint)
        pick_b = dot_t(one_hot(c == code_b), joint)
        rr = iota((32, rows8), 0)
        packed_a = jnp.zeros((32, ca), F32)
        packed_b = jnp.zeros((32, cb), F32)
        for q in range(PIECES):
            mine_a = jnp.where(bits(rr, 2, 2) == q, pick_a, 0.0).astype(BF16)
            packed_a += dot(mine_a, normed[:, q * ca:(q + 1) * ca])
            mine_b = jnp.where(bits(rr, 3, 2) == q, pick_b, 0.0).astype(BF16)
            packed_b += dot(mine_b, normed[:, base_b + q * cb:base_b + (q + 1) * cb])
        pack_a[...] = packed_a.astype(BF16).reshape(E_WIN, PIECES * CAP, ca)
        pack_b[...] = packed_b.astype(BF16)
        unit_a[layer, y] = pack_a[expert]
        unit_b[layer, x] = pack_b[...]

        def direct_a(step):
            to = (y + step) % side
            return remote(pack_a.at[to // (side // E_WIN)], unit_a.at[layer, y], dir_send.at[0, step],
                          dir_recv.at[layer, 0, step], at(to, x))

        def direct_b(step):
            return remote(pack_b, unit_b.at[layer, x], dir_send.at[1, step],
                          dir_recv.at[layer, 1, step], at(y, (x + step) % side))

        for step in range(1, side):
            direct_a(step).start()
            direct_b(step).start()

        logits = dot_t(normed[...], router_all[layer])
        chosen = [jnp.sum(h[:, :logits.shape[1]] * logits, axis=-1, keepdims=True) for h in hot]
        gates = [jax.nn.sigmoid(chosen[0] - chosen[1]), jax.nn.sigmoid(chosen[1] - chosen[0])]

        for step in range(1, side):
            direct_a(step).wait()
        ga[layer, x] = dot(swap(side * 16, lg, 2, 2), unit_a[layer].reshape(side * 16, ca)).astype(BF16).reshape(
            PIECES, bundle, ca)

        def hop(k, go, step):
            slot = shift(k, -go * step)
            ref = ga.at[layer, slot, k] if k < PIECES else gb.at[layer, slot, k - PIECES]
            return remote(ref, ref, ring_send.at[k, way(go)], ring_recv.at[layer, k, way(go), step], beside(k, go))

        for k in range(PIECES):
            for go in (1, -1):
                hop(k, go, 0).start()
        for step in range(1, side):
            direct_b(step).wait()
        gb[layer, y] = dot(swap(side * 32, lg, 3, 2), unit_b[layer].reshape(side * 32, cb)).astype(BF16).reshape(
            PIECES, 2 * bundle, cb)
        for k in range(PIECES, 2 * PIECES):
            for go in (1, -1):
                hop(k, go, 0).start()

        def ring_step(step, c):
            for k, go in streams:
                hop(k, go, step - 1).wait()
                hop(k, go, step).start()
            return c

        lax.fori_loop(1, half_way - 1, ring_step, 0)
        for k, go in streams:
            hop(k, go, half_way - 2).wait()
            if hops(k, go) == half_way:
                hop(k, go, half_way - 1).start()

        for kind in (2, 3, 4):
            param_wait(kind, layer)
        rows = side * bundle
        order = swap(rows, lg, lg, 2)
        own_half = pl.ds(pl.multiple_of(expert * bundle, bundle), bundle)
        g = u = None
        for q in order_of:
            for k in (q, q + PIECES):
                for go in (1, -1):
                    if hops(k, go) == half_way:
                        hop(k, go, half_way - 1).wait()
            lhs_a = ga[layer, :, q].reshape(rows, ca)
            at_a = pl.ds(q * ca, ca)
            lhs_b = dot(order, gb[layer, :, q, own_half].reshape(rows, cb)).astype(BF16)
            at_b = pl.ds(base_b + q * cb, cb)
            part_g = dot(lhs_a, gate_all[layer, at_a]) + dot(lhs_b, gate_all[layer, at_b])
            part_u = dot(lhs_a, up_all[layer, at_a]) + dot(lhs_b, up_all[layer, at_b])
            g, u = (part_g, part_u) if g is None else (g + part_g, u + part_u)
        hidden = (g * jax.nn.sigmoid(g) * u).astype(BF16)
        hidden_b = dot(order, hidden).astype(BF16)

        def pass_on(k, go, step):
            if k < PIECES:
                src = ta.at[k, shift(k, go * hops(k, go))] if step == 0 else ra.at[layer, step - 1, way(go), k]
                dst = ra.at[layer, step, way(go), k]
            else:
                q = k - PIECES
                src = sb.at[way(go), q] if step == 0 else rb.at[layer, step - 1, way(go), q]
                dst = rb.at[layer, step, way(go), q]
            return remote(src, dst, sum_send.at[k, way(go)], sum_recv.at[layer, k, way(go), step], beside(k, go))

        def add_own(k, go, step):
            slot = shift(k, go * (hops(k, go) - step))
            if k < PIECES:
                at_ = (layer, step - 1, way(go), k)
                ra[at_] = (ra[at_].astype(F32) + ta[k, slot].astype(F32)).astype(BF16)
            else:
                at_ = (layer, step - 1, way(go), k - PIECES, own_half)
                rb[at_] = (rb[at_].astype(F32) + tb[k - PIECES, slot].astype(F32)).astype(BF16)

        for q in order_of:
            term = dot(hidden, down_all[layer, :, q * ca:(q + 1) * ca]).astype(BF16)
            ta[q] = term.reshape(side, bundle, ca)
            for go in (1, -1):
                pass_on(q, go, 0).start()
            term = dot(hidden_b, down_all[layer, :, base_b + q * cb:base_b + (q + 1) * cb]).astype(BF16)
            tb[q] = term.reshape(side, bundle, cb)
            for go in (1, -1):
                k = q + PIECES
                sb[way(go), q, own_half] = tb[q, shift(k, go * hops(k, go))]
                pass_on(k, go, 0).start()

        for step in range(1, half_way + 1):
            for k, go in streams:
                if step <= hops(k, go):
                    pass_on(k, go, step - 1).wait()
                if step < hops(k, go):
                    add_own(k, go, step)
                    pass_on(k, go, step).start()

        def arrived(k, ref, *at_):
            return sum(ref[(layer, hops(k, go) - 1, way(go), k % PIECES) + at_].astype(F32) for go in (1, -1))

        for q in range(PIECES):
            fa[q] = (arrived(q, ra) + ta[q, x].astype(F32)).astype(BF16)
            fb[q] = arrived(q + PIECES, rb).astype(BF16)
            fb[q, own_half] = (arrived(q + PIECES, rb, own_half) + tb[q, y].astype(F32)).astype(BF16)
        wa[...] = dot(swap(side * 16, 2, lg, 2), fa[...].reshape(side * 16, ca)).astype(BF16).reshape(side, PIECES * CAP, ca)
        wb[...] = dot(swap(side * 32, 3, lg, 2), fb[...].reshape(side * 32, cb)).astype(BF16).reshape(
            side, PIECES * 2 * CAP, cb)
        va[layer, y] = wa[y]
        vb[layer, x] = wb[x]

        def back_a(step):
            to = (y + step) % side
            return remote(wa.at[to], va.at[layer, y], back_send.at[0, step], back_recv.at[layer, 0, step], at(to, x))

        def back_b(step):
            to = (x + step) % side
            return remote(wb.at[to], vb.at[layer, x], back_send.at[1, step], back_recv.at[layer, 1, step], at(y, to))

        for step in range(1, side):
            back_a(step).start()
            back_b(step).start()
        for step in range(1, side):
            back_a(step).wait()
            back_b(step).wait()

        half = side // E_WIN
        out_a = jnp.concatenate(
            [sum(va[layer, n * half + j].astype(F32) for j in range(half)) for n in range(E_WIN)], axis=0)
        out_b = sum(vb[layer, j].astype(F32) for j in range(side))
        lane = iota((rows8, 32), 1)
        code_a = (bits(lane, 4, 1) * CAP + bits(lane, 0, 2)).astype(F32)
        code_b = bits(lane, 0, 3).astype(F32)
        weight_a = sum(jnp.where(code_a == c, g_, 0.0) for c, g_ in zip(code, gates))
        weight_b = sum(jnp.where(code_b == c, g_, 0.0) for c, g_ in zip(code, gates))
        for q in range(PIECES):
            for weight, which, value, begin, wide in (
                    (weight_a, bits(lane, 2, 2), out_a, q * ca, ca),
                    (weight_b, bits(lane, 3, 2), out_b, base_b + q * cb, cb)):
                moe = dot(jnp.where(which == q, weight, 0.0), value, precision=lax.Precision.HIGHEST)
                columns = slice(begin, begin + wide)
                stream[:, columns] = (stream[:, columns].astype(F32) + moe).astype(BF16)
        return carry

    lax.fori_loop(0, 2, one_layer, 0)
    out[0] = stream[...]
    for copy in sends:
        copy.wait_send()


def body(tokens, expert_ids, norm_gain, router, w_gate, w_up, w_down):
    side = math.isqrt(lax.axis_size("expert"))
    block, width = tokens.shape[1:]
    ff = w_gate.shape[-1]
    ca = width * 2 // 3 // PIECES
    cb = width // 3 // PIECES
    bundle = side * CAP
    ids = jnp.swapaxes(expert_ids[0], 1, 2)
    router_t = jnp.swapaxes(router, 1, 2)
    gain = norm_gain[:, None, :]
    dma = pltpu.SemaphoreType.DMA
    hbm = pl.BlockSpec(memory_space=pl.ANY)
    scratch = [
        pltpu.VMEM((block, width), BF16),
        pltpu.VMEM((block, width), BF16),
        pltpu.VMEM((2, 2, block), jnp.int32),
        pltpu.VMEM((2, 1, width), BF16),
        pltpu.VMEM((2, router.shape[-1], width), BF16),
        pltpu.VMEM((2, width, ff), BF16),
        pltpu.VMEM((2, width, ff), BF16),
        pltpu.VMEM((2, ff, width), BF16),
        pltpu.VMEM((E_WIN, PIECES * CAP, ca), BF16),
        pltpu.VMEM((PIECES * E_WIN * CAP, cb), BF16),
        pltpu.VMEM((2, side, PIECES * CAP, ca), BF16),
        pltpu.VMEM((2, side, PIECES * E_WIN * CAP, cb), BF16),
        pltpu.VMEM((2, side, PIECES, bundle, ca), BF16),
        pltpu.VMEM((2, side, PIECES, E_WIN * bundle, cb), BF16),
        pltpu.VMEM((PIECES, side, bundle, ca), BF16),
        pltpu.VMEM((PIECES, side, bundle, cb), BF16),
        pltpu.VMEM((2, PIECES, E_WIN * bundle, cb), BF16),
        pltpu.VMEM((2, side // 2, 2, PIECES, bundle, ca), BF16),
        pltpu.VMEM((2, side // 2, 2, PIECES, E_WIN * bundle, cb), BF16),
        pltpu.VMEM((PIECES, bundle, ca), BF16),
        pltpu.VMEM((PIECES, E_WIN * bundle, cb), BF16),
        pltpu.VMEM((side, PIECES * CAP, ca), BF16),
        pltpu.VMEM((side, PIECES * E_WIN * CAP, cb), BF16),
        pltpu.VMEM((2, side, PIECES * CAP, ca), BF16),
        pltpu.VMEM((2, side, PIECES * E_WIN * CAP, cb), BF16),
        dma,
        dma((6, 2)),
        dma((6,)),
        dma((2, side)),
        dma((2, 2, side)),
        dma((2 * PIECES, 2)),
        dma((2, 2 * PIECES, 2, side // 2)),
        dma((2, side)),
        dma((2, 2, side)),
        dma((2 * PIECES, 2)),
        dma((2, 2 * PIECES, 2, side // 2)),
    ]
    return pl.pallas_call(
        functools.partial(kernel, side),
        out_shape=jax.ShapeDtypeStruct((1, block, width), BF16),
        in_specs=[hbm] * 7,
        out_specs=pl.BlockSpec(memory_space=pltpu.VMEM),
        scratch_shapes=scratch,
        compiler_params=pltpu.CompilerParams(
            collective_id=0, has_side_effects=True, vmem_limit_bytes=60 * 1024 * 1024),
        name="moe_step",
    )(tokens, ids, gain, router_t, w_gate, w_up, w_down)


def solution(mesh):
    in_specs = (
        P(None, ("groups", "expert"), None),
        P("section", None, ("groups", "expert"), None),
        P("section", None),
        P("section", None, None),
        P("section", None, "expert"),
        P("section", None, "expert"),
        P("section", "expert", None),
    )
    out_specs = P("section", ("groups", "expert"), None)
    return jax.shard_map(body, mesh=mesh, in_specs=in_specs, out_specs=out_specs, check_vma=False)
```

```python
import functools
import math

import jax
import jax.numpy as jnp
from jax import lax
from jax.experimental import pallas as pl
from jax.experimental.pallas import tpu as pltpu
from jax.sharding import PartitionSpec as P

E_WIN = 2
CAP = 4
PIECES = 4
WAVES = 2
EPS = 1e-05
MESH = pl.DeviceIdType.MESH
F32, BF16 = jnp.float32, jnp.bfloat16


def bits(value, low, count):
    return lax.bitwise_and(lax.shift_right_logical(value, low), (1 << count) - 1)


def iota(shape, dim):
    return lax.broadcasted_iota(jnp.int32, shape, dim)


def one_hot(condition):
    return jnp.where(condition, 1.0, 0.0).astype(BF16)


def swap(rows, high, low, tail):
    to, frm = iota((rows, rows), 0), iota((rows, rows), 1)
    to_l, to_h = bits(to, tail + high, low), bits(to, tail, high)
    frm_h, frm_l = bits(frm, tail + low, high), bits(frm, tail, low)
    same = (bits(to, 0, tail) == bits(frm, 0, tail)) & (to_l == frm_l) & (to_h == frm_h)
    return one_hot(same)


def dot(a, b, **kw):
    return jnp.dot(a, b, preferred_element_type=F32, **kw)


def dot_t(a, b):
    return lax.dot_general(a, b, (((1,), (1,)), ((), ())), preferred_element_type=F32)


def kernel(side, tokens, ids, gain, router, w_gate, w_up, w_down, out,
           stream, normed, ids_all, gain_all, router_all, gate_all, up_all, down_all,
           pack_a, pack_b, unit_a, unit_b, ga, gb, ta, tb, sb, ra, rb, fa, fb, wa, wb, va, vb,
           own_sem, param_sem, param_send, dir_send, dir_recv, ring_send, ring_recv,
           back_send, back_recv, sum_send, sum_recv):
    lg = side.bit_length() - 1
    width = stream.shape[1]
    ca, cb = ga.shape[-1], gb.shape[-1]
    base_b = PIECES * ca
    s = lax.axis_index("section")
    me = lax.axis_index("expert")
    y, x = me // side, me % side
    expert = y // (side // E_WIN)
    bundle = side * CAP

    def at(yy, xx):
        return {"expert": yy * side + xx}

    other = {"section": 1 - s}
    params = ((gain, gain_all), (router, router_all), (w_gate, gate_all), (w_up, up_all), (w_down, down_all))

    def remote(src, dst, send, recv, device):
        return pltpu.make_async_remote_copy(src_ref=src, dst_ref=dst, send_sem=send, recv_sem=recv,
                                            device_id=device, device_id_type=MESH)

    barrier = pltpu.get_barrier_semaphore()
    pl.semaphore_signal(barrier, inc=1, device_id=other, device_id_type=MESH)
    for step in range(1, side):
        pl.semaphore_signal(barrier, inc=1, device_id=at(y, (x + step) % side), device_id_type=MESH)
        pl.semaphore_signal(barrier, inc=1, device_id=at((y + step) % side, x), device_id_type=MESH)
    token_copy = pltpu.make_async_copy(tokens.at[s], stream, own_sem)
    token_copy.start()
    pltpu.make_async_copy(ids.at[s], ids_all.at[s], param_sem.at[5, s]).start()
    for kind, (src, dst) in enumerate(params):
        pltpu.make_async_copy(src.at[0], dst.at[s], param_sem.at[kind, s]).start()

    sb[...] = jnp.zeros_like(sb)
    token_copy.wait()
    pl.semaphore_wait(barrier, 2 * side - 1)

    sends = [remote(ids.at[1 - s], ids_all.at[s], param_send.at[5], param_sem.at[5, s], other)]
    for kind, (src, dst) in enumerate(params):
        sends.append(remote(src.at[0], dst.at[s], param_send.at[kind], param_sem.at[kind, s], other))
    for copy in sends:
        copy.start()

    def param_wait(kind, layer):
        src, dst = params[kind]
        pltpu.make_async_copy(src.at[0], dst.at[layer], param_sem.at[kind, layer]).wait()

    half_way = side // 2

    def hops(k, go):
        return half_way if (k % 2 == 0) == (go > 0) else half_way - 1

    def place(k):
        return x if k < PIECES else y

    def beside(k, go):
        return at(y, (x + side + go) % side) if k < PIECES else at((y + side + go) % side, x)

    def shift(k, steps):
        return (place(k) + side + steps) % side

    waves = range(WAVES)
    per = PIECES // WAVES

    def of_wave(w):
        return [(q + base, go) for q in range(w * per, (w + 1) * per) for base in (0, PIECES) for go in (1, -1)]

    far_first = sorted(range(1, side), key=lambda step: -min(step, side - step))

    def way(go):
        return 0 if go > 0 else 1

    def one_layer(layer, carry):
        pltpu.make_async_copy(ids.at[s], ids_all.at[layer], param_sem.at[5, layer]).wait()
        param_wait(0, layer)
        param_wait(1, layer)
        values = stream[...].astype(F32)
        scale = lax.rsqrt(jnp.mean(values * values, axis=-1, keepdims=True) + EPS)
        normed[...] = (values * scale * gain_all[layer].astype(F32)).astype(BF16)
        id_block = ids_all[layer]
        rows8 = id_block.shape[1]
        eye = one_hot(iota((rows8, rows8), 0) == iota((rows8, rows8), 1))
        id_block = dot_t(eye, id_block.astype(F32).astype(BF16))
        lanes = iota((rows8, 128), 1)
        named = [id_block[:, k:k + 1] for k in range(2)]
        lane_f = lanes.astype(F32)
        hot = [jnp.where(lane_f == n, 1.0, 0.0) for n in named]
        earlier = jnp.where(iota((rows8, rows8), 0) > iota((rows8, rows8), 1), 1.0, 0.0)
        before = dot(earlier.astype(BF16), (hot[0] + hot[1]).astype(BF16))
        code = [jnp.sum(h * before, axis=-1, keepdims=True) + n * CAP
                for h, n in zip(hot, named)]
        joint = sum(jnp.where(lane_f == c, 1.0, 0.0) for c in code).astype(BF16)
        r = iota((16, 128), 0)
        c = iota((16, 128), 1)
        pick_a = dot_t(one_hot(c == bits(r, 3, 1) * CAP + bits(r, 0, 2)), joint)
        pick_b = dot_t(one_hot(c == bits(r, 0, 3)), joint)
        rr = iota((16, rows8), 0)
        mine_a = [jnp.where(bits(rr, 2, 1) == q, pick_a, 0.0).astype(BF16) for q in range(per)]
        mine_b = [jnp.where(bits(rr, 3, 1) == q, pick_b, 0.0).astype(BF16) for q in range(per)]

        def direct_a(w, step):
            to = (y + step) % side
            return remote(pack_a.at[w, to // (side // E_WIN)], unit_a.at[layer, w, y], dir_send.at[0, w, step],
                          dir_recv.at[layer, 0, w, step], at(to, x))

        def direct_b(w, step):
            return remote(pack_b.at[w], unit_b.at[layer, w, x], dir_send.at[1, w, step],
                          dir_recv.at[layer, 1, w, step], at(y, (x + step) % side))

        for w in waves:
            packed_a = sum(dot(mine_a[q], normed[:, (w * per + q) * ca:(w * per + q + 1) * ca]) for q in range(per))
            pack_a[w] = packed_a.astype(BF16).reshape(E_WIN, per * CAP, ca)
            packed_b = sum(dot(mine_b[q], normed[:, base_b + (w * per + q) * cb:base_b + (w * per + q + 1) * cb])
                           for q in range(per))
            pack_b[w] = packed_b.astype(BF16)
            for step in far_first:
                direct_a(w, step).start()
                direct_b(w, step).start()
            unit_a[layer, w, y] = pack_a[w, expert]
            unit_b[layer, w, x] = pack_b[w]

        logits = dot_t(normed[...], router_all[layer])
        chosen = [jnp.sum(h[:, :logits.shape[1]] * logits, axis=-1, keepdims=True) for h in hot]
        gates = [jax.nn.sigmoid(chosen[0] - chosen[1]), jax.nn.sigmoid(chosen[1] - chosen[0])]

        def hop(k, go, step):
            slot = shift(k, -go * step)
            ref = ga.at[layer, slot, k] if k < PIECES else gb.at[layer, slot, k - PIECES]
            return remote(ref, ref, ring_send.at[k, way(go)], ring_recv.at[layer, k, way(go), step], beside(k, go))

        for w in waves:
            now = pl.ds(w * per, per)
            for step in range(1, side):
                direct_a(w, step).wait()
            ga[layer, x, now] = dot(swap(side * 8, lg, 1, 2), unit_a[layer, w].reshape(side * 8, ca)).astype(
                BF16).reshape(per, bundle, ca)
            for k, go in of_wave(w):
                if k < PIECES:
                    hop(k, go, 0).start()
            for step in range(1, side):
                direct_b(w, step).wait()
            gb[layer, y, now] = dot(swap(side * 16, lg, 2, 2), unit_b[layer, w].reshape(side * 16, cb)).astype(
                BF16).reshape(per, 2 * bundle, cb)
            for k, go in of_wave(w):
                if k >= PIECES:
                    hop(k, go, 0).start()

        def ring_step(step, c):
            for w in waves:
                for k, go in of_wave(w):
                    hop(k, go, step - 1).wait()
                    hop(k, go, step).start()
            return c

        lax.fori_loop(1, half_way - 1, ring_step, 0)
        for w in waves:
            for k, go in of_wave(w):
                hop(k, go, half_way - 2).wait()
                if hops(k, go) == half_way:
                    hop(k, go, half_way - 1).start()

        for kind in (2, 3, 4):
            param_wait(kind, layer)
        rows = side * bundle
        order = swap(rows, lg, lg, 2)
        own_half = pl.ds(pl.multiple_of(expert * bundle, bundle), bundle)
        g = u = None
        for q in range(PIECES):
            for k in (q, q + PIECES):
                for go in (1, -1):
                    if hops(k, go) == half_way:
                        hop(k, go, half_way - 1).wait()
            lhs_a = ga[layer, :, q].reshape(rows, ca)
            at_a = pl.ds(q * ca, ca)
            lhs_b = dot(order, gb[layer, :, q, own_half].reshape(rows, cb)).astype(BF16)
            at_b = pl.ds(base_b + q * cb, cb)
            part_g = dot(lhs_a, gate_all[layer, at_a]) + dot(lhs_b, gate_all[layer, at_b])
            part_u = dot(lhs_a, up_all[layer, at_a]) + dot(lhs_b, up_all[layer, at_b])
            g, u = (part_g, part_u) if g is None else (g + part_g, u + part_u)
        hidden = (g * jax.nn.sigmoid(g) * u).astype(BF16)
        hidden_b = dot(order, hidden).astype(BF16)

        def pass_on(k, go, step):
            if k < PIECES:
                src = ta.at[k, shift(k, go * hops(k, go))] if step == 0 else ra.at[layer, step - 1, way(go), k]
                dst = ra.at[layer, step, way(go), k]
            else:
                q = k - PIECES
                src = sb.at[way(go), q] if step == 0 else rb.at[layer, step - 1, way(go), q]
                dst = rb.at[layer, step, way(go), q]
            return remote(src, dst, sum_send.at[k, way(go)], sum_recv.at[layer, k, way(go), step], beside(k, go))

        def add_own(k, go, step):
            slot = shift(k, go * (hops(k, go) - step))
            if k < PIECES:
                at_ = (layer, step - 1, way(go), k)
                ra[at_] = (ra[at_].astype(F32) + ta[k, slot].astype(F32)).astype(BF16)
            else:
                at_ = (layer, step - 1, way(go), k - PIECES, own_half)
                rb[at_] = (rb[at_].astype(F32) + tb[k - PIECES, slot].astype(F32)).astype(BF16)

        for q in range(PIECES):
            term = dot(hidden, down_all[layer, :, q * ca:(q + 1) * ca]).astype(BF16)
            ta[q] = term.reshape(side, bundle, ca)
            for go in (1, -1):
                pass_on(q, go, 0).start()
            term = dot(hidden_b, down_all[layer, :, base_b + q * cb:base_b + (q + 1) * cb]).astype(BF16)
            tb[q] = term.reshape(side, bundle, cb)
            for go in (1, -1):
                k = q + PIECES
                sb[way(go), q, own_half] = tb[q, shift(k, go * hops(k, go))]
                pass_on(k, go, 0).start()

        def arrived(k, ref, *at_):
            return sum(ref[(layer, hops(k, go) - 1, way(go), k % PIECES) + at_].astype(F32) for go in (1, -1))

        def back_a(w, step):
            to = (y + step) % side
            return remote(wa.at[w, to], va.at[layer, w, y], back_send.at[0, w, step],
                          back_recv.at[layer, 0, w, step], at(to, x))

        def back_b(w, step):
            to = (x + step) % side
            return remote(wb.at[w, to], vb.at[layer, w, x], back_send.at[1, w, step],
                          back_recv.at[layer, 1, w, step], at(y, to))

        for step in range(1, half_way + 1):
            for w in waves:
                for k, go in of_wave(w):
                    if step <= hops(k, go):
                        pass_on(k, go, step - 1).wait()
                    if step < hops(k, go):
                        add_own(k, go, step)
                        pass_on(k, go, step).start()
                if step < half_way:
                    continue
                for q in range(w * per, (w + 1) * per):
                    fa[q] = (arrived(q, ra) + ta[q, x].astype(F32)).astype(BF16)
                    fb[q] = arrived(q + PIECES, rb).astype(BF16)
                    fb[q, own_half] = (arrived(q + PIECES, rb, own_half) + tb[q, y].astype(F32)).astype(BF16)
                now = pl.ds(w * per, per)
                wa[w] = dot(swap(side * 8, 1, lg, 2), fa[now].reshape(side * 8, ca)).astype(BF16).reshape(
                    side, per * CAP, ca)
                wb[w] = dot(swap(side * 16, 2, lg, 2), fb[now].reshape(side * 16, cb)).astype(BF16).reshape(
                    side, per * 2 * CAP, cb)
                for step_ in far_first:
                    back_a(w, step_).start()
                    back_b(w, step_).start()
                va[layer, w, y] = wa[w, y]
                vb[layer, w, x] = wb[w, x]

        half = side // E_WIN
        lane = iota((rows8, 16), 1)
        code_a = (bits(lane, 3, 1) * CAP + bits(lane, 0, 2)).astype(F32)
        code_b = bits(lane, 0, 3).astype(F32)
        weight_a = sum(jnp.where(code_a == c, g_, 0.0) for c, g_ in zip(code, gates))
        weight_b = sum(jnp.where(code_b == c, g_, 0.0) for c, g_ in zip(code, gates))
        for w in waves:
            for step in range(1, side):
                back_a(w, step).wait()
                back_b(w, step).wait()
            out_a = jnp.concatenate(
                [sum(va[layer, w, n * half + j].astype(F32) for j in range(half)) for n in range(E_WIN)], axis=0)
            out_b = sum(vb[layer, w, j].astype(F32) for j in range(side))
            for q in range(per):
                piece = w * per + q
                for weight, which, value, begin, wide in (
                        (weight_a, bits(lane, 2, 1), out_a, piece * ca, ca),
                        (weight_b, bits(lane, 3, 1), out_b, base_b + piece * cb, cb)):
                    moe = dot(jnp.where(which == q, weight, 0.0), value, precision=lax.Precision.HIGHEST)
                    columns = slice(begin, begin + wide)
                    stream[:, columns] = (stream[:, columns].astype(F32) + moe).astype(BF16)
        return carry

    lax.fori_loop(0, 2, one_layer, 0)
    out[0] = stream[...]
    for copy in sends:
        copy.wait_send()


def body(tokens, expert_ids, norm_gain, router, w_gate, w_up, w_down):
    side = math.isqrt(lax.axis_size("expert"))
    block, width = tokens.shape[1:]
    ff = w_gate.shape[-1]
    ca = width * 2 // 3 // PIECES
    cb = width // 3 // PIECES
    bundle = side * CAP
    per = PIECES // WAVES
    ids = jnp.swapaxes(expert_ids[0], 1, 2)
    router_t = jnp.swapaxes(router, 1, 2)
    gain = norm_gain[:, None, :]
    dma = pltpu.SemaphoreType.DMA
    hbm = pl.BlockSpec(memory_space=pl.ANY)
    scratch = [
        pltpu.VMEM((block, width), BF16),
        pltpu.VMEM((block, width), BF16),
        pltpu.VMEM((2, 2, block), jnp.int32),
        pltpu.VMEM((2, 1, width), BF16),
        pltpu.VMEM((2, router.shape[-1], width), BF16),
        pltpu.VMEM((2, width, ff), BF16),
        pltpu.VMEM((2, width, ff), BF16),
        pltpu.VMEM((2, ff, width), BF16),
        pltpu.VMEM((WAVES, E_WIN, per * CAP, ca), BF16),
        pltpu.VMEM((WAVES, per * E_WIN * CAP, cb), BF16),
        pltpu.VMEM((2, WAVES, side, per * CAP, ca), BF16),
        pltpu.VMEM((2, WAVES, side, per * E_WIN * CAP, cb), BF16),
        pltpu.VMEM((2, side, PIECES, bundle, ca), BF16),
        pltpu.VMEM((2, side, PIECES, E_WIN * bundle, cb), BF16),
        pltpu.VMEM((PIECES, side, bundle, ca), BF16),
        pltpu.VMEM((PIECES, side, bundle, cb), BF16),
        pltpu.VMEM((2, PIECES, E_WIN * bundle, cb), BF16),
        pltpu.VMEM((2, side // 2, 2, PIECES, bundle, ca), BF16),
        pltpu.VMEM((2, side // 2, 2, PIECES, E_WIN * bundle, cb), BF16),
        pltpu.VMEM((PIECES, bundle, ca), BF16),
        pltpu.VMEM((PIECES, E_WIN * bundle, cb), BF16),
        pltpu.VMEM((WAVES, side, per * CAP, ca), BF16),
        pltpu.VMEM((WAVES, side, per * E_WIN * CAP, cb), BF16),
        pltpu.VMEM((2, WAVES, side, per * CAP, ca), BF16),
        pltpu.VMEM((2, WAVES, side, per * E_WIN * CAP, cb), BF16),
        dma,
        dma((6, 2)),
        dma((6,)),
        dma((2, WAVES, side)),
        dma((2, 2, WAVES, side)),
        dma((2 * PIECES, 2)),
        dma((2, 2 * PIECES, 2, side // 2)),
        dma((2, WAVES, side)),
        dma((2, 2, WAVES, side)),
        dma((2 * PIECES, 2)),
        dma((2, 2 * PIECES, 2, side // 2)),
    ]
    return pl.pallas_call(
        functools.partial(kernel, side),
        out_shape=jax.ShapeDtypeStruct((1, block, width), BF16),
        in_specs=[hbm] * 7,
        out_specs=pl.BlockSpec(memory_space=pltpu.VMEM),
        scratch_shapes=scratch,
        compiler_params=pltpu.CompilerParams(
            collective_id=0, has_side_effects=True, vmem_limit_bytes=60 * 1024 * 1024),
        name="moe_step",
    )(tokens, ids, gain, router_t, w_gate, w_up, w_down)


def solution(mesh):
    in_specs = (
        P(None, ("groups", "expert"), None),
        P("section", None, ("groups", "expert"), None),
        P("section", None),
        P("section", None, None),
        P("section", None, "expert"),
        P("section", None, "expert"),
        P("section", "expert", None),
    )
    out_specs = P("section", ("groups", "expert"), None)
    return jax.shard_map(body, mesh=mesh, in_specs=in_specs, out_specs=out_specs, check_vma=False)
```

```python
import functools
import math

import jax
import jax.numpy as jnp
from jax import lax
from jax.experimental import pallas as pl
from jax.experimental.pallas import tpu as pltpu
from jax.sharding import PartitionSpec as P

E_WIN = 2
CAP = 4
PIECES = 4
WAVES = 2
EPS = 1e-05
MESH = pl.DeviceIdType.MESH
F32, BF16 = jnp.float32, jnp.bfloat16


def bits(value, low, count):
    return lax.bitwise_and(lax.shift_right_logical(value, low), (1 << count) - 1)


def iota(shape, dim):
    return lax.broadcasted_iota(jnp.int32, shape, dim)


def one_hot(condition):
    return jnp.where(condition, 1.0, 0.0).astype(BF16)


def swap(rows, high, low, tail):
    to, frm = iota((rows, rows), 0), iota((rows, rows), 1)
    to_l, to_h = bits(to, tail + high, low), bits(to, tail, high)
    frm_h, frm_l = bits(frm, tail + low, high), bits(frm, tail, low)
    same = (bits(to, 0, tail) == bits(frm, 0, tail)) & (to_l == frm_l) & (to_h == frm_h)
    return one_hot(same)


def dot(a, b, **kw):
    return jnp.dot(a, b, preferred_element_type=F32, **kw)


def dot_t(a, b):
    return lax.dot_general(a, b, (((1,), (1,)), ((), ())), preferred_element_type=F32)


def kernel(side, tokens, ids, gain, router, w_gate, w_up, w_down, out,
           stream, normed, ids_all, gain_all, router_all, pair_all, down_all,
           pack_a, pack_b, unit_a, unit_b, ga, gb, ta, tb, ra, rb, fa, fb, wa, wb, va, vb,
           own_sem, param_sem, param_send, dir_send, dir_recv, ring_send, ring_recv,
           back_send, back_recv, sum_send, sum_recv):
    lg = side.bit_length() - 1
    width = stream.shape[1]
    ca, cb = ga.shape[-1], gb.shape[-1]
    base_b = PIECES * ca
    s = lax.axis_index("section")
    me = lax.axis_index("expert")
    y, x = lax.div(me, side), lax.rem(me, side)
    expert = lax.div(y, side // E_WIN)
    bundle = side * CAP

    def at(yy, xx):
        return {"expert": yy * side + xx}

    other = {"section": 1 - s}
    ff = down_all.shape[1]
    params = (
        (gain, lambda n: gain_all.at[n]),
        (router, lambda n: router_all.at[n]),
        (w_gate, lambda n: pair_all.at[n, :, pl.ds(0, ff)]),
        (w_up, lambda n: pair_all.at[n, :, pl.ds(ff, ff)]),
        (w_down, lambda n: down_all.at[n]),
    )

    def remote(src, dst, send, recv, device):
        return pltpu.make_async_remote_copy(src_ref=src, dst_ref=dst, send_sem=send, recv_sem=recv,
                                            device_id=device, device_id_type=MESH)

    barrier = pltpu.get_barrier_semaphore()
    pl.semaphore_signal(barrier, inc=1, device_id=other, device_id_type=MESH)
    for step in range(1, side):
        pl.semaphore_signal(barrier, inc=1, device_id=at(y, (x + step) % side), device_id_type=MESH)
        pl.semaphore_signal(barrier, inc=1, device_id=at((y + step) % side, x), device_id_type=MESH)
    token_copy = pltpu.make_async_copy(tokens.at[s], stream, own_sem)
    token_copy.start()
    pltpu.make_async_copy(ids.at[s], ids_all.at[s], param_sem.at[5, s]).start()
    for kind, (src, dst) in enumerate(params):
        pltpu.make_async_copy(src.at[0], dst(s), param_sem.at[kind, s]).start()

    token_copy.wait()
    pl.semaphore_wait(barrier, 2 * side - 1)

    sends = [remote(ids.at[1 - s], ids_all.at[s], param_send.at[5], param_sem.at[5, s], other)]
    for kind, (src, dst) in enumerate(params):
        sends.append(remote(src.at[0], dst(s), param_send.at[kind], param_sem.at[kind, s], other))
    for copy in sends:
        copy.start()

    def param_wait(kind, layer):
        src, dst = params[kind]
        pltpu.make_async_copy(src.at[0], dst(layer), param_sem.at[kind, layer]).wait()

    half_way = side // 2
    half = side // E_WIN
    per = PIECES // WAVES
    lp = per.bit_length() - 1
    unit = per * E_WIN * CAP
    ways = [(kind, is_far) for kind in range(2) for is_far in (True, False)]

    def heading(q, is_far):
        turn = 1 - 2 * lax.rem(q, 2)
        return turn if is_far else -turn

    def hops(is_far):
        return half_way if is_far else half_way - 1

    def way(go):
        return lax.div(1 - go, 2)

    def wrapped(value):
        return lax.rem(value + side, side)

    def beside(kind, go):
        return at(wrapped(y + go), x) if kind else at(y, wrapped(x + go))

    def shift(kind, steps):
        return wrapped((y if kind else x) + steps)

    def reaches(part, go, first, last):
        hit = None
        for j in range(first, last + 1):
            same = lax.div(wrapped(y + go * j), half) == part
            hit = same if hit is None else jnp.logical_or(hit, same)
        return hit

    def parts(go, first, last):
        each = [reaches(part, go, first, last) for part in range(E_WIN)]
        return jnp.logical_and(*each), lax.div(wrapped(y + go * first), half)

    def rows_of(part):
        return pl.ds(pl.multiple_of(part * bundle, bundle), bundle)

    def columns_of(kind, q):
        wide = cb if kind else ca
        return pl.ds(pl.multiple_of(q * wide + (base_b if kind else 0), 128), wide)

    def loop(first, last, step):
        def run(i, carry):
            step(i)
            return carry
        lax.fori_loop(first, last, run, 0)

    def wait_all(like, *sems):
        for sem in sems:
            pltpu.make_async_copy(like, like, sem).wait()

    def begin(hop):
        make, out_, _ = hop
        if out_ is None:
            make(None).start()
            return
        pl.when(out_[0])(lambda: make(pl.ds(0, E_WIN * bundle)).start())
        pl.when(jnp.logical_not(out_[0]))(lambda: make(rows_of(out_[1])).start())

    def finish(hop):
        make, out_, in_ = hop
        if out_ is None:
            make(None).wait()
            return
        everything, one = pl.ds(0, E_WIN * bundle), pl.ds(0, bundle)
        for which, end in ((out_, "wait_send"), (in_, "wait_recv")):
            pl.when(which[0])(lambda end=end: getattr(make(everything), end)())
            pl.when(jnp.logical_not(which[0]))(lambda end=end: getattr(make(one), end)())

    def one_layer(layer, carry):
        pltpu.make_async_copy(ids.at[s], ids_all.at[layer], param_sem.at[5, layer]).wait()
        param_wait(0, layer)
        param_wait(1, layer)
        values = stream[...].astype(F32)
        scale = lax.rsqrt(jnp.mean(values * values, axis=-1, keepdims=True) + EPS)
        normed[...] = (values * scale * gain_all[layer].astype(F32)).astype(BF16)
        id_block = ids_all[layer]
        rows8 = id_block.shape[1]
        eye = one_hot(iota((rows8, rows8), 0) == iota((rows8, rows8), 1))
        id_block = dot_t(eye, id_block.astype(F32).astype(BF16))
        lanes = iota((rows8, 128), 1)
        named = [id_block[:, k:k + 1] for k in range(2)]
        lane_f = lanes.astype(F32)
        hot = [jnp.where(lane_f == n, 1.0, 0.0) for n in named]
        earlier = jnp.where(iota((rows8, rows8), 0) > iota((rows8, rows8), 1), 1.0, 0.0)
        before = dot(earlier.astype(BF16), (hot[0] + hot[1]).astype(BF16))
        code = [jnp.sum(h * before, axis=-1, keepdims=True) + n * CAP
                for h, n in zip(hot, named)]
        joint = sum(jnp.where(lane_f == c, 1.0, 0.0) for c in code).astype(BF16)
        r = iota((unit, 128), 0)
        c = iota((unit, 128), 1)
        pick_a = dot_t(one_hot(c == bits(r, 2 + lp, 1) * CAP + bits(r, 0, 2)), joint)
        pick_b = dot_t(one_hot(c == bits(r, 0, 3)), joint)
        rr = iota((unit, rows8), 0)
        mine_a = [jnp.where(bits(rr, 2, lp) == q, pick_a, 0.0).astype(BF16) for q in range(per)]
        mine_b = [jnp.where(bits(rr, 3, lp) == q, pick_b, 0.0).astype(BF16) for q in range(per)]

        def direct(w, step, kind):
            to_y, to_x = wrapped(y + step), wrapped(x + step)
            if kind:
                return remote(pack_b.at[w], unit_b.at[layer, w, x], dir_send.at[1, w],
                              dir_recv.at[1, w], at(y, to_x))
            return remote(pack_a.at[w, lax.div(to_y, half)], unit_a.at[layer, w, y], dir_send.at[0, w],
                          dir_recv.at[0, w], at(to_y, x))

        def pack(w):
            first = w * per
            packed_a = sum(dot(mine_a[q], normed[:, columns_of(0, first + q)]) for q in range(per))
            pack_a[w] = packed_a.astype(BF16).reshape(E_WIN, per * CAP, ca)
            packed_b = sum(dot(mine_b[q], normed[:, columns_of(1, first + q)]) for q in range(per))
            pack_b[w] = packed_b.astype(BF16)

            def send(i):
                for kind in range(2):
                    direct(w, 1 + lax.rem(i + half_way - 1, side - 1), kind).start()

            loop(0, side - 1, send)
            unit_a[layer, w, y] = pack_a[w, expert]
            unit_b[layer, w, x] = pack_b[w]

        loop(0, WAVES, pack)

        logits = dot_t(normed[...], router_all[layer])
        chosen = [jnp.sum(h[:, :logits.shape[1]] * logits, axis=-1, keepdims=True) for h in hot]
        gates = [jax.nn.sigmoid(chosen[0] - chosen[1]), jax.nn.sigmoid(chosen[1] - chosen[0])]

        def hop(kind, q, is_far, step):
            go = heading(q, is_far)
            slot = shift(kind, -go * step)
            k = kind * PIECES + q
            sems = (ring_send.at[k, way(go)], ring_recv.at[k, way(go), step])

            def make(rows):
                ref = gb.at[layer, slot, q, rows] if kind else ga.at[layer, slot, q]
                return remote(ref, ref, *sems, beside(kind, go))

            left = hops(is_far) - step
            return (make, parts(go, 1, left), parts(go, 0, left - 1)) if kind else (make, None, None)

        def spread(w):
            now = pl.ds(w * per, per)
            wait_all(unit_a.at[layer, w, pl.ds(0, side - 1)], dir_send.at[0, w], dir_recv.at[0, w])
            ga[layer, x, now] = dot(
                swap(side * per * CAP, lg, lp, 2), unit_a[layer, w].reshape(side * per * CAP, ca)).astype(
                    BF16).reshape(per, bundle, ca)

            def start(kind):
                def go_on(i):
                    for is_far in (True, False):
                        begin(hop(kind, w * per + i, is_far, 0))
                loop(0, per, go_on)

            start(0)
            wait_all(unit_b.at[layer, w, pl.ds(0, side - 1)], dir_send.at[1, w], dir_recv.at[1, w])
            gb[layer, y, now] = dot(
                swap(side * unit, lg, lp + 1, 2), unit_b[layer, w].reshape(side * unit, cb)).astype(BF16).reshape(
                    per, 2 * bundle, cb)
            start(1)

        loop(0, WAVES, spread)

        for step in range(1, half_way):
            def ring_step(q, step=step):
                for kind, is_far in ways:
                    finish(hop(kind, q, is_far, step - 1))
                    if step < hops(is_far):
                        begin(hop(kind, q, is_far, step))
            loop(0, PIECES, ring_step)

        for kind in (2, 3, 4):
            param_wait(kind, layer)
        rows = side * bundle
        order = swap(rows, lg, lg, 2)
        own_half = rows_of(expert)

        def products(q, both):
            for kind in range(2):
                finish(hop(kind, q, True, half_way - 1))
            lhs_a = ga[layer, :, q].reshape(rows, ca)
            lhs_b = dot(order, gb[layer, :, q, own_half].reshape(rows, cb)).astype(BF16)
            return both + dot(lhs_a, pair_all[layer, columns_of(0, q)]) + dot(lhs_b, pair_all[layer, columns_of(1, q)])

        both = lax.fori_loop(0, PIECES, products, jnp.zeros((rows, 2 * ff), F32))
        g, u = both[:, :ff], both[:, ff:]
        hidden = (g * jax.nn.sigmoid(g) * u).astype(BF16)
        hidden_b = dot(order, hidden).astype(BF16)

        def pass_on(kind, q, is_far, step):
            go = heading(q, is_far)
            slot = shift(kind, go * hops(is_far))
            k = kind * PIECES + q
            sems = (sum_send.at[k, way(go)], sum_recv.at[k, way(go), step])

            def make(rows):
                if kind:
                    src = tb.at[q, slot] if step == 0 else rb.at[layer, step - 1, way(go), q, rows]
                    return remote(src, rb.at[layer, step, way(go), q, rows], *sems, beside(kind, go))
                src = ta.at[q, slot] if step == 0 else ra.at[layer, step - 1, way(go), q]
                return remote(src, ra.at[layer, step, way(go), q], *sems, beside(kind, go))

            return (make, parts(-go, 0, step), parts(-go, 1, step + 1)) if kind else (make, None, None)

        def add_own(kind, q, is_far, step):
            go = heading(q, is_far)
            slot = shift(kind, go * (hops(is_far) - step))
            if not kind:
                at_ = (layer, step - 1, way(go), q)
                ra[at_] = (ra[at_].astype(F32) + ta[q, slot].astype(F32)).astype(BF16)
                return
            at_ = (layer, step - 1, way(go), q, own_half)
            came = reaches(expert, -go, 1, step)

            def add():
                rb[at_] = (rb[at_].astype(F32) + tb[q, slot].astype(F32)).astype(BF16)

            def put():
                rb[at_] = tb[q, slot]

            pl.when(came)(add)
            pl.when(jnp.logical_not(came))(put)

        def clear(q, is_far):
            go = heading(q, is_far)
            for part in range(E_WIN):
                def zero(part=part):
                    rb[layer, hops(is_far) - 1, way(go), q, rows_of(part)] = jnp.zeros((bundle, cb), BF16)
                pl.when(jnp.logical_not(reaches(part, -go, 1, hops(is_far))))(zero)

        def begin_own(q, is_far):
            pass_on(1, q, is_far, 0)[0](own_half).start()

        def terms(q):
            ta[q] = dot(hidden, down_all[layer, :, columns_of(0, q)]).astype(BF16).reshape(side, bundle, ca)
            for is_far in (True, False):
                begin(pass_on(0, q, is_far, 0))
            tb[q] = dot(hidden_b, down_all[layer, :, columns_of(1, q)]).astype(BF16).reshape(side, bundle, cb)
            for is_far in (True, False):
                begin_own(q, is_far)
                clear(q, is_far)

        loop(0, PIECES, terms)

        for step in range(1, half_way):
            def sum_step(q, step=step):
                for kind, is_far in ways:
                    finish(pass_on(kind, q, is_far, step - 1))
                    if step < hops(is_far):
                        add_own(kind, q, is_far, step)
                        begin(pass_on(kind, q, is_far, step))
            loop(0, PIECES, sum_step)

        def back(w, step):
            to_y, to_x = wrapped(y + step), wrapped(x + step)
            return (remote(wa.at[w, to_y], va.at[layer, w, y], back_send.at[0, w],
                           back_recv.at[0, w], at(to_y, x)),
                    remote(wb.at[w, to_x], vb.at[layer, w, x], back_send.at[1, w],
                           back_recv.at[1, w], at(y, to_x)))

        def arrived(ref, q, *at_):
            return sum(ref[(layer, hops(is_far) - 1, way(heading(q, is_far)), q) + at_].astype(F32)
                       for is_far in (True, False))

        def give_back(w):
            def last(i):
                q = w * per + i
                for kind in range(2):
                    finish(pass_on(kind, q, True, half_way - 1))
                fa[q] = (arrived(ra, q) + ta[q, x].astype(F32)).astype(BF16)
                fb[q] = arrived(rb, q).astype(BF16)
                fb[q, own_half] = (arrived(rb, q, own_half) + tb[q, y].astype(F32)).astype(BF16)

            loop(0, per, last)
            now = pl.ds(w * per, per)
            wa[w] = dot(swap(side * per * CAP, lp, lg, 2), fa[now].reshape(side * per * CAP, ca)).astype(
                BF16).reshape(side, per * CAP, ca)
            wb[w] = dot(swap(side * unit, lp + 1, lg, 2), fb[now].reshape(side * unit, cb)).astype(BF16).reshape(
                side, unit, cb)

            def send(i):
                for copy in back(w, 1 + lax.rem(i + half_way - 1, side - 1)):
                    copy.start()

            loop(0, side - 1, send)
            va[layer, w, y] = wa[w, y]
            vb[layer, w, x] = wb[w, x]

        loop(0, WAVES, give_back)

        lane = iota((rows8, unit), 1)
        code_a = (bits(lane, 2 + lp, 1) * CAP + bits(lane, 0, 2)).astype(F32)
        code_b = bits(lane, 0, 3).astype(F32)
        weight_a = sum(jnp.where(code_a == c, g_, 0.0) for c, g_ in zip(code, gates))
        weight_b = sum(jnp.where(code_b == c, g_, 0.0) for c, g_ in zip(code, gates))

        def add_up(w):
            wait_all(va.at[layer, w, pl.ds(0, side - 1)], back_send.at[0, w], back_recv.at[0, w])
            wait_all(vb.at[layer, w, pl.ds(0, side - 1)], back_send.at[1, w], back_recv.at[1, w])
            out_a = jnp.concatenate(
                [sum(va[layer, w, n * half + j].astype(F32) for j in range(half)) for n in range(E_WIN)], axis=0)
            out_b = sum(vb[layer, w, j].astype(F32) for j in range(side))
            for q in range(per):
                for weight, which, value, kind in ((weight_a, bits(lane, 2, lp), out_a, 0),
                                                   (weight_b, bits(lane, 3, lp), out_b, 1)):
                    moe = dot(jnp.where(which == q, weight, 0.0), value, precision=lax.Precision.HIGHEST)
                    columns = columns_of(kind, w * per + q)
                    stream[:, columns] = (stream[:, columns].astype(F32) + moe).astype(BF16)

        loop(0, WAVES, add_up)
        return carry

    lax.fori_loop(0, 2, one_layer, 0)
    out[0] = stream[...]
    for copy in sends:
        copy.wait_send()


def body(tokens, expert_ids, norm_gain, router, w_gate, w_up, w_down):
    side = math.isqrt(lax.axis_size("expert"))
    block, width = tokens.shape[1:]
    ff = w_gate.shape[-1]
    ca = width * 2 // 3 // PIECES
    cb = width // 3 // PIECES
    bundle = side * CAP
    per = PIECES // WAVES
    ids = jnp.swapaxes(expert_ids[0], 1, 2)
    router_t = jnp.swapaxes(router, 1, 2)
    gain = norm_gain[:, None, :]
    dma = pltpu.SemaphoreType.DMA
    hbm = pl.BlockSpec(memory_space=pl.ANY)
    scratch = [
        pltpu.VMEM((block, width), BF16),
        pltpu.VMEM((block, width), BF16),
        pltpu.VMEM((2, 2, block), jnp.int32),
        pltpu.VMEM((2, 1, width), BF16),
        pltpu.VMEM((2, router.shape[-1], width), BF16),
        pltpu.VMEM((2, width, 2 * ff), BF16),
        pltpu.VMEM((2, ff, width), BF16),
        pltpu.VMEM((WAVES, E_WIN, per * CAP, ca), BF16),
        pltpu.VMEM((WAVES, per * E_WIN * CAP, cb), BF16),
        pltpu.VMEM((2, WAVES, side, per * CAP, ca), BF16),
        pltpu.VMEM((2, WAVES, side, per * E_WIN * CAP, cb), BF16),
        pltpu.VMEM((2, side, PIECES, bundle, ca), BF16),
        pltpu.VMEM((2, side, PIECES, E_WIN * bundle, cb), BF16),
        pltpu.VMEM((PIECES, side, bundle, ca), BF16),
        pltpu.VMEM((PIECES, side, bundle, cb), BF16),
        pltpu.VMEM((2, side // 2, 2, PIECES, bundle, ca), BF16),
        pltpu.VMEM((2, side // 2, 2, PIECES, E_WIN * bundle, cb), BF16),
        pltpu.VMEM((PIECES, bundle, ca), BF16),
        pltpu.VMEM((PIECES, E_WIN * bundle, cb), BF16),
        pltpu.VMEM((WAVES, side, per * CAP, ca), BF16),
        pltpu.VMEM((WAVES, side, per * E_WIN * CAP, cb), BF16),
        pltpu.VMEM((2, WAVES, side, per * CAP, ca), BF16),
        pltpu.VMEM((2, WAVES, side, per * E_WIN * CAP, cb), BF16),
        dma,
        dma((6, 2)),
        dma((6,)),
        dma((2, WAVES)),
        dma((2, WAVES)),
        dma((2 * PIECES, 2)),
        dma((2 * PIECES, 2, side // 2)),
        dma((2, WAVES)),
        dma((2, WAVES)),
        dma((2 * PIECES, 2)),
        dma((2 * PIECES, 2, side // 2)),
    ]
    return pl.pallas_call(
        functools.partial(kernel, side),
        out_shape=jax.ShapeDtypeStruct((1, block, width), BF16),
        in_specs=[hbm] * 7,
        out_specs=pl.BlockSpec(memory_space=pltpu.VMEM),
        scratch_shapes=scratch,
        compiler_params=pltpu.CompilerParams(
            collective_id=0, has_side_effects=True, vmem_limit_bytes=60 * 1024 * 1024),
        name="moe_step",
    )(tokens, ids, gain, router_t, w_gate, w_up, w_down)


def solution(mesh):
    in_specs = (
        P(None, ("groups", "expert"), None),
        P("section", None, ("groups", "expert"), None),
        P("section", None),
        P("section", None, None),
        P("section", None, "expert"),
        P("section", None, "expert"),
        P("section", "expert", None),
    )
    out_specs = P("section", ("groups", "expert"), None)
    return jax.shard_map(body, mesh=mesh, in_specs=in_specs, out_specs=out_specs, check_vma=False)
```

```python
import functools
import math

import jax
import jax.numpy as jnp
from jax import lax
from jax.experimental import pallas as pl
from jax.experimental.pallas import tpu as pltpu
from jax.sharding import PartitionSpec as P

E_WIN = 2
CAP = 4
PIECES = 4
WAVES = 2
EPS = 1e-05
MESH = pl.DeviceIdType.MESH
F32, BF16 = jnp.float32, jnp.bfloat16


def bits(value, low, count):
    return lax.bitwise_and(lax.shift_right_logical(value, low), (1 << count) - 1)


def iota(shape, dim):
    return lax.broadcasted_iota(jnp.int32, shape, dim)


def one_hot(condition):
    return jnp.where(condition, 1.0, 0.0).astype(BF16)


def swap(rows, high, low, tail):
    to, frm = iota((rows, rows), 0), iota((rows, rows), 1)
    to_l, to_h = bits(to, tail + high, low), bits(to, tail, high)
    frm_h, frm_l = bits(frm, tail + low, high), bits(frm, tail, low)
    same = (bits(to, 0, tail) == bits(frm, 0, tail)) & (to_l == frm_l) & (to_h == frm_h)
    return one_hot(same)


def dot(a, b, **kw):
    return jnp.dot(a, b, preferred_element_type=F32, **kw)


def dot_t(a, b):
    return lax.dot_general(a, b, (((1,), (1,)), ((), ())), preferred_element_type=F32)


def kernel(side, tokens, ids, gain, router, w_gate, w_up, w_down, out,
           stream, normed, ids_all, gain_all, router_all, pair_all, down_all,
           pack_a, pack_b, unit_a, unit_b, ga, gb, ta, tb, ra, rb, fa, fb, wa, wb, va, vb,
           own_sem, param_sem, param_send, dir_send, dir_recv, ring_send, ring_recv,
           back_send, back_recv, sum_send, sum_recv):
    lg = side.bit_length() - 1
    width = stream.shape[1]
    ca, cb = ga.shape[-1], gb.shape[-1]
    base_b = PIECES * ca
    s = lax.axis_index("section")
    me = lax.axis_index("expert")
    y, x = lax.div(me, side), lax.rem(me, side)
    expert = lax.div(y, side // E_WIN)
    bundle = side * CAP

    def at(yy, xx):
        return {"expert": yy * side + xx}

    other = {"section": 1 - s}
    ff = down_all.shape[1]
    params = (
        (gain, lambda n: gain_all.at[n]),
        (router, lambda n: router_all.at[n]),
        (w_gate, lambda n: pair_all.at[n, :, pl.ds(0, ff)]),
        (w_up, lambda n: pair_all.at[n, :, pl.ds(ff, ff)]),
        (w_down, lambda n: down_all.at[n]),
    )

    def remote(src, dst, send, recv, device):
        return pltpu.make_async_remote_copy(src_ref=src, dst_ref=dst, send_sem=send, recv_sem=recv,
                                            device_id=device, device_id_type=MESH)

    barrier = pltpu.get_barrier_semaphore()
    pl.semaphore_signal(barrier, inc=1, device_id=other, device_id_type=MESH)
    for step in range(1, side):
        pl.semaphore_signal(barrier, inc=1, device_id=at(y, (x + step) % side), device_id_type=MESH)
        pl.semaphore_signal(barrier, inc=1, device_id=at((y + step) % side, x), device_id_type=MESH)
    token_copy = pltpu.make_async_copy(tokens.at[s], stream, own_sem)
    token_copy.start()
    pltpu.make_async_copy(ids.at[s], ids_all.at[s], param_sem.at[5, s]).start()
    for kind, (src, dst) in enumerate(params):
        pltpu.make_async_copy(src.at[0], dst(s), param_sem.at[kind, s]).start()

    token_copy.wait()
    pl.semaphore_wait(barrier, 2 * side - 1)

    sends = [remote(ids.at[1 - s], ids_all.at[s], param_send.at[5], param_sem.at[5, s], other)]
    for kind, (src, dst) in enumerate(params):
        sends.append(remote(src.at[0], dst(s), param_send.at[kind], param_sem.at[kind, s], other))
    for copy in sends:
        copy.start()

    def param_wait(kind, layer):
        src, dst = params[kind]
        pltpu.make_async_copy(src.at[0], dst(layer), param_sem.at[kind, layer]).wait()

    half_way = side // 2
    half = side // E_WIN
    per = PIECES // WAVES
    lp = per.bit_length() - 1
    unit = per * E_WIN * CAP
    ways = [(kind, is_far) for is_far in (True, False) for kind in range(2)]

    def heading(q, is_far):
        turn = 1 - 2 * lax.rem(q, 2)
        return turn if is_far else -turn

    def hops(is_far):
        return half_way if is_far else half_way - 1

    def way(go):
        return lax.div(1 - go, 2)

    def wrapped(value):
        return lax.rem(value + side, side)

    def beside(kind, go):
        return at(wrapped(y + go), x) if kind else at(y, wrapped(x + go))

    def shift(kind, steps):
        return wrapped((y if kind else x) + steps)

    def reaches(part, go, first, last):
        hit = None
        for j in range(first, last + 1):
            same = lax.div(wrapped(y + go * j), half) == part
            hit = same if hit is None else jnp.logical_or(hit, same)
        return hit

    def parts(go, first, last):
        each = [reaches(part, go, first, last) for part in range(E_WIN)]
        return jnp.logical_and(*each), lax.div(wrapped(y + go * first), half)

    def rows_of(part):
        return pl.ds(pl.multiple_of(part * bundle, bundle), bundle)

    def columns_of(kind, q):
        wide = cb if kind else ca
        return pl.ds(pl.multiple_of(q * wide + (base_b if kind else 0), 128), wide)

    def loop(first, last, step):
        def run(i, carry):
            step(i)
            return carry
        lax.fori_loop(first, last, run, 0)

    def wait_all(like, *sems):
        for sem in sems:
            pltpu.make_async_copy(like, like, sem).wait()

    def begin(hop):
        make, out_, _ = hop
        if out_ is None:
            make(None).start()
            return
        pl.when(out_[0])(lambda: make(pl.ds(0, E_WIN * bundle)).start())
        pl.when(jnp.logical_not(out_[0]))(lambda: make(rows_of(out_[1])).start())

    def finish(hop):
        make, out_, in_ = hop
        if out_ is None:
            make(None).wait()
            return
        everything, one = pl.ds(0, E_WIN * bundle), pl.ds(0, bundle)
        for which, end in ((out_, "wait_send"), (in_, "wait_recv")):
            pl.when(which[0])(lambda end=end: getattr(make(everything), end)())
            pl.when(jnp.logical_not(which[0]))(lambda end=end: getattr(make(one), end)())

    def one_layer(layer, carry):
        pltpu.make_async_copy(ids.at[s], ids_all.at[layer], param_sem.at[5, layer]).wait()
        param_wait(0, layer)
        param_wait(1, layer)
        values = stream[...].astype(F32)
        scale = lax.rsqrt(jnp.mean(values * values, axis=-1, keepdims=True) + EPS)
        normed[...] = (values * scale * gain_all[layer].astype(F32)).astype(BF16)
        id_block = ids_all[layer]
        rows8 = id_block.shape[1]
        eye = one_hot(iota((rows8, rows8), 0) == iota((rows8, rows8), 1))
        id_block = dot_t(eye, id_block.astype(F32).astype(BF16))
        lanes = iota((rows8, 128), 1)
        named = [id_block[:, k:k + 1] for k in range(2)]
        lane_f = lanes.astype(F32)
        hot = [jnp.where(lane_f == n, 1.0, 0.0) for n in named]
        earlier = jnp.where(iota((rows8, rows8), 0) > iota((rows8, rows8), 1), 1.0, 0.0)
        before = dot(earlier.astype(BF16), (hot[0] + hot[1]).astype(BF16))
        code = [jnp.sum(h * before, axis=-1, keepdims=True) + n * CAP
                for h, n in zip(hot, named)]
        joint = sum(jnp.where(lane_f == c, 1.0, 0.0) for c in code).astype(BF16)
        r = iota((unit, 128), 0)
        c = iota((unit, 128), 1)
        pick_a = dot_t(one_hot(c == bits(r, 2 + lp, 1) * CAP + bits(r, 0, 2)), joint)
        pick_b = dot_t(one_hot(c == bits(r, 0, 3)), joint)
        rr = iota((unit, rows8), 0)
        mine_a = [jnp.where(bits(rr, 2, lp) == q, pick_a, 0.0).astype(BF16) for q in range(per)]
        mine_b = [jnp.where(bits(rr, 3, lp) == q, pick_b, 0.0).astype(BF16) for q in range(per)]

        def direct(w, step, kind):
            to_y, to_x = wrapped(y + step), wrapped(x + step)
            if kind:
                return remote(pack_b.at[w], unit_b.at[layer, w, x], dir_send.at[1, w],
                              dir_recv.at[1, w], at(y, to_x))
            return remote(pack_a.at[w, lax.div(to_y, half)], unit_a.at[layer, w, y], dir_send.at[0, w],
                          dir_recv.at[0, w], at(to_y, x))

        def pack(w):
            first = w * per
            packed_a = sum(dot(mine_a[q], normed[:, columns_of(0, first + q)]) for q in range(per))
            pack_a[w] = packed_a.astype(BF16).reshape(E_WIN, per * CAP, ca)
            packed_b = sum(dot(mine_b[q], normed[:, columns_of(1, first + q)]) for q in range(per))
            pack_b[w] = packed_b.astype(BF16)

            def send(i):
                for kind in range(2):
                    direct(w, 1 + lax.rem(i + half_way - 1, side - 1), kind).start()

            loop(0, side - 1, send)
            unit_a[layer, w, y] = pack_a[w, expert]
            unit_b[layer, w, x] = pack_b[w]

        loop(0, WAVES, pack)

        logits = dot_t(normed[...], router_all[layer])
        chosen = [jnp.sum(h[:, :logits.shape[1]] * logits, axis=-1, keepdims=True) for h in hot]
        gates = [jax.nn.sigmoid(chosen[0] - chosen[1]), jax.nn.sigmoid(chosen[1] - chosen[0])]

        def hop(kind, q, is_far, step):
            go = heading(q, is_far)
            slot = shift(kind, -go * step)
            k = kind * PIECES + q
            sems = (ring_send.at[k, way(go)], ring_recv.at[k, step + (0 if is_far else half_way)])

            def make(rows):
                ref = gb.at[layer, slot, q, rows] if kind else ga.at[layer, slot, q]
                return remote(ref, ref, *sems, beside(kind, go))

            left = hops(is_far) - step
            return (make, parts(go, 1, left), parts(go, 0, left - 1)) if kind else (make, None, None)

        def spread(w):
            now = pl.ds(w * per, per)
            wait_all(unit_a.at[layer, w, pl.ds(0, side - 1)], dir_send.at[0, w], dir_recv.at[0, w])
            ga[layer, x, now] = dot(
                swap(side * per * CAP, lg, lp, 2), unit_a[layer, w].reshape(side * per * CAP, ca)).astype(
                    BF16).reshape(per, bundle, ca)

            def start(kind):
                def go_on(i):
                    for is_far in (True, False):
                        begin(hop(kind, w * per + i, is_far, 0))
                loop(0, per, go_on)

            start(0)
            wait_all(unit_b.at[layer, w, pl.ds(0, side - 1)], dir_send.at[1, w], dir_recv.at[1, w])
            gb[layer, y, now] = dot(
                swap(side * unit, lg, lp + 1, 2), unit_b[layer, w].reshape(side * unit, cb)).astype(BF16).reshape(
                    per, 2 * bundle, cb)
            start(1)

        loop(0, WAVES, spread)

        for step in range(1, half_way):
            def ring_step(q, step=step):
                for kind, is_far in ways:
                    finish(hop(kind, q, is_far, step - 1))
                    if step < hops(is_far):
                        begin(hop(kind, q, is_far, step))
            loop(0, PIECES, ring_step)

        for kind in (2, 3, 4):
            param_wait(kind, layer)
        rows = side * bundle
        order = swap(rows, lg, lg, 2)
        own_half = rows_of(expert)

        def products(q, both):
            for kind in range(2):
                finish(hop(kind, q, True, half_way - 1))
            lhs_a = ga[layer, :, q].reshape(rows, ca)
            lhs_b = dot(order, gb[layer, :, q, own_half].reshape(rows, cb)).astype(BF16)
            return both + dot(lhs_a, pair_all[layer, columns_of(0, q)]) + dot(lhs_b, pair_all[layer, columns_of(1, q)])

        both = lax.fori_loop(0, PIECES, products, jnp.zeros((rows, 2 * ff), F32))
        g, u = both[:, :ff], both[:, ff:]
        hidden = (g * jax.nn.sigmoid(g) * u).astype(BF16)
        hidden_b = dot(order, hidden).astype(BF16)

        def pass_on(kind, q, is_far, step):
            go = heading(q, is_far)
            slot = shift(kind, go * hops(is_far))
            k = kind * PIECES + q
            sems = (sum_send.at[k, way(go)], sum_recv.at[k, step + (0 if is_far else half_way)])

            def make(rows):
                if kind:
                    src = tb.at[q, slot] if step == 0 else rb.at[layer, step - 1, way(go), q, rows]
                    return remote(src, rb.at[layer, step, way(go), q, rows], *sems, beside(kind, go))
                src = ta.at[q, slot] if step == 0 else ra.at[layer, step - 1, way(go), q]
                return remote(src, ra.at[layer, step, way(go), q], *sems, beside(kind, go))

            return (make, parts(-go, 0, step), parts(-go, 1, step + 1)) if kind else (make, None, None)

        def add_own(kind, q, is_far, step):
            go = heading(q, is_far)
            slot = shift(kind, go * (hops(is_far) - step))
            if not kind:
                at_ = (layer, step - 1, way(go), q)
                ra[at_] = (ra[at_].astype(F32) + ta[q, slot].astype(F32)).astype(BF16)
                return
            at_ = (layer, step - 1, way(go), q, own_half)
            came = reaches(expert, -go, 1, step)

            def add():
                rb[at_] = (rb[at_].astype(F32) + tb[q, slot].astype(F32)).astype(BF16)

            def put():
                rb[at_] = tb[q, slot]

            pl.when(came)(add)
            pl.when(jnp.logical_not(came))(put)

        def clear(q, is_far):
            go = heading(q, is_far)
            for part in range(E_WIN):
                def zero(part=part):
                    rb[layer, hops(is_far) - 1, way(go), q, rows_of(part)] = jnp.zeros((bundle, cb), BF16)
                pl.when(jnp.logical_not(reaches(part, -go, 1, hops(is_far))))(zero)

        def begin_own(q, is_far):
            pass_on(1, q, is_far, 0)[0](own_half).start()

        def terms(q):
            ta[q] = dot(hidden, down_all[layer, :, columns_of(0, q)]).astype(BF16).reshape(side, bundle, ca)
            for is_far in (True, False):
                begin(pass_on(0, q, is_far, 0))
            tb[q] = dot(hidden_b, down_all[layer, :, columns_of(1, q)]).astype(BF16).reshape(side, bundle, cb)
            for is_far in (True, False):
                begin_own(q, is_far)
                clear(q, is_far)

        loop(0, PIECES, terms)

        for step in range(1, half_way):
            def sum_step(q, step=step):
                for kind, is_far in ways:
                    finish(pass_on(kind, q, is_far, step - 1))
                    if step < hops(is_far):
                        add_own(kind, q, is_far, step)
                        begin(pass_on(kind, q, is_far, step))
            loop(0, PIECES, sum_step)

        def back(w, step):
            to_y, to_x = wrapped(y + step), wrapped(x + step)
            return (remote(wa.at[w, to_y], va.at[layer, w, y], back_send.at[0, w],
                           back_recv.at[0, w], at(to_y, x)),
                    remote(wb.at[w, to_x], vb.at[layer, w, x], back_send.at[1, w],
                           back_recv.at[1, w], at(y, to_x)))

        def arrived(ref, q, *at_):
            return sum(ref[(layer, hops(is_far) - 1, way(heading(q, is_far)), q) + at_].astype(F32)
                       for is_far in (True, False))

        def give_back(w):
            def last(i):
                q = w * per + i
                for kind in range(2):
                    finish(pass_on(kind, q, True, half_way - 1))
                fa[q] = (arrived(ra, q) + ta[q, x].astype(F32)).astype(BF16)
                fb[q] = arrived(rb, q).astype(BF16)
                fb[q, own_half] = (arrived(rb, q, own_half) + tb[q, y].astype(F32)).astype(BF16)

            loop(0, per, last)
            now = pl.ds(w * per, per)
            wa[w] = dot(swap(side * per * CAP, lp, lg, 2), fa[now].reshape(side * per * CAP, ca)).astype(
                BF16).reshape(side, per * CAP, ca)
            wb[w] = dot(swap(side * unit, lp + 1, lg, 2), fb[now].reshape(side * unit, cb)).astype(BF16).reshape(
                side, unit, cb)

            def send(i):
                for copy in back(w, 1 + lax.rem(i + half_way - 1, side - 1)):
                    copy.start()

            loop(0, side - 1, send)
            va[layer, w, y] = wa[w, y]
            vb[layer, w, x] = wb[w, x]

        loop(0, WAVES, give_back)

        lane = iota((rows8, unit), 1)
        code_a = (bits(lane, 2 + lp, 1) * CAP + bits(lane, 0, 2)).astype(F32)
        code_b = bits(lane, 0, 3).astype(F32)
        weight_a = sum(jnp.where(code_a == c, g_, 0.0) for c, g_ in zip(code, gates))
        weight_b = sum(jnp.where(code_b == c, g_, 0.0) for c, g_ in zip(code, gates))

        def add_up(w):
            wait_all(va.at[layer, w, pl.ds(0, side - 1)], back_send.at[0, w], back_recv.at[0, w])
            wait_all(vb.at[layer, w, pl.ds(0, side - 1)], back_send.at[1, w], back_recv.at[1, w])
            out_a = jnp.concatenate(
                [sum(va[layer, w, n * half + j].astype(F32) for j in range(half)) for n in range(E_WIN)], axis=0)
            out_b = sum(vb[layer, w, j].astype(F32) for j in range(side))
            for q in range(per):
                for weight, which, value, kind in ((weight_a, bits(lane, 2, lp), out_a, 0),
                                                   (weight_b, bits(lane, 3, lp), out_b, 1)):
                    moe = dot(jnp.where(which == q, weight, 0.0), value, precision=lax.Precision.HIGHEST)
                    columns = columns_of(kind, w * per + q)
                    stream[:, columns] = (stream[:, columns].astype(F32) + moe).astype(BF16)

        loop(0, WAVES, add_up)
        return carry

    lax.fori_loop(0, 2, one_layer, 0)
    out[0] = stream[...]
    for copy in sends:
        copy.wait_send()


def body(tokens, expert_ids, norm_gain, router, w_gate, w_up, w_down):
    side = math.isqrt(lax.axis_size("expert"))
    block, width = tokens.shape[1:]
    ff = w_gate.shape[-1]
    ca = width * 2 // 3 // PIECES
    cb = width // 3 // PIECES
    bundle = side * CAP
    per = PIECES // WAVES
    ids = jnp.swapaxes(expert_ids[0], 1, 2)
    router_t = jnp.swapaxes(router, 1, 2)
    gain = norm_gain[:, None, :]
    dma = pltpu.SemaphoreType.DMA
    hbm = pl.BlockSpec(memory_space=pl.ANY)
    scratch = [
        pltpu.VMEM((block, width), BF16),
        pltpu.VMEM((block, width), BF16),
        pltpu.VMEM((2, 2, block), jnp.int32),
        pltpu.VMEM((2, 1, width), BF16),
        pltpu.VMEM((2, router.shape[-1], width), BF16),
        pltpu.VMEM((2, width, 2 * ff), BF16),
        pltpu.VMEM((2, ff, width), BF16),
        pltpu.VMEM((WAVES, E_WIN, per * CAP, ca), BF16),
        pltpu.VMEM((WAVES, per * E_WIN * CAP, cb), BF16),
        pltpu.VMEM((2, WAVES, side, per * CAP, ca), BF16),
        pltpu.VMEM((2, WAVES, side, per * E_WIN * CAP, cb), BF16),
        pltpu.VMEM((2, side, PIECES, bundle, ca), BF16),
        pltpu.VMEM((2, side, PIECES, E_WIN * bundle, cb), BF16),
        pltpu.VMEM((PIECES, side, bundle, ca), BF16),
        pltpu.VMEM((PIECES, side, bundle, cb), BF16),
        pltpu.VMEM((2, side // 2, 2, PIECES, bundle, ca), BF16),
        pltpu.VMEM((2, side // 2, 2, PIECES, E_WIN * bundle, cb), BF16),
        pltpu.VMEM((PIECES, bundle, ca), BF16),
        pltpu.VMEM((PIECES, E_WIN * bundle, cb), BF16),
        pltpu.VMEM((WAVES, side, per * CAP, ca), BF16),
        pltpu.VMEM((WAVES, side, per * E_WIN * CAP, cb), BF16),
        pltpu.VMEM((2, WAVES, side, per * CAP, ca), BF16),
        pltpu.VMEM((2, WAVES, side, per * E_WIN * CAP, cb), BF16),
        dma,
        dma((6, 2)),
        dma((6,)),
        dma((2, WAVES)),
        dma((2, WAVES)),
        dma((2 * PIECES, 2)),
        dma((2 * PIECES, side - 1)),
        dma((2, WAVES)),
        dma((2, WAVES)),
        dma((2 * PIECES, 2)),
        dma((2 * PIECES, side - 1)),
    ]
    return pl.pallas_call(
        functools.partial(kernel, side),
        out_shape=jax.ShapeDtypeStruct((1, block, width), BF16),
        in_specs=[hbm] * 7,
        out_specs=pl.BlockSpec(memory_space=pltpu.VMEM),
        scratch_shapes=scratch,
        compiler_params=pltpu.CompilerParams(
            collective_id=0, has_side_effects=True, vmem_limit_bytes=60 * 1024 * 1024),
        name="moe_step",
    )(tokens, ids, gain, router_t, w_gate, w_up, w_down)


def solution(mesh):
    in_specs = (
        P(None, ("groups", "expert"), None),
        P("section", None, ("groups", "expert"), None),
        P("section", None),
        P("section", None, None),
        P("section", None, "expert"),
        P("section", None, "expert"),
        P("section", "expert", None),
    )
    out_specs = P("section", ("groups", "expert"), None)
    return jax.shard_map(body, mesh=mesh, in_specs=in_specs, out_specs=out_specs, check_vma=False)
```
